16 devices in a mesh: data: 16 (over z, y, x, core).
Axes of the slice: x: 2, y: 2, z: 2, core: 2. Of those that a mesh axis runs over, the one named last changes fastest.
Arguments:
- x_in: bfloat16 [65536, 1024], P('data')
- d_out: bfloat16 [65536, 1024], P('data')
- w_stack: bfloat16 [4, 1024, 1024], replicated
- a_old: float32 [4, 1024, 1024], replicated
- s_old: float32 [4, 1024, 1024], replicated
- a_inv: float32 [4, 1024, 1024], replicated
- s_inv: float32 [4, 1024, 1024], replicated
Outputs:
- output 1: float32 [4, 1024, 1024], replicated
- output 2: float32 [4, 1024, 1024], replicated
- output 3: float32 [4, 1024, 1024], replicated
All inputs are finite; a program needn't handle non-finite values.
Results may differ from the reference program's by a relative error of at most 0.00138593.
Values are sent between devices in bfloat16 or wider.
A program may use at most 1 GiB of HBM per device.

```python
import jax
import jax.numpy as jnp
from jax import lax

D = 1024
LAYERS = 4
TOK_DEV = 4096
GROUP = 16
RANK = 64
TOKENS = TOK_DEV * GROUP
RHO = 0.75
ERF_SCALE = 0.7071067811865476
PDF_SCALE = 0.3989422804014327


def gelu_fwd(z_val):
    return 0.5 * z_val * (1.0 + lax.erf(z_val * ERF_SCALE))


def gelu_slope(z_val):
    return 0.5 * (1.0 + lax.erf(z_val * ERF_SCALE)) + z_val * jnp.exp(-0.5 * z_val * z_val) * PDF_SCALE


def tok_gram(lhs_rows, rhs_rows):
    return lax.dot_general(lhs_rows, rhs_rows, (((0,), (0,)), ((), ())), preferred_element_type=jnp.float32)


def sharded_rows(key_list, base_size, own_size, mix_lo, mix_hi, scale_lo, scale_hi):
    noise_rows = jax.random.normal(key_list[0], (GROUP, TOK_DEV, D), jnp.float32)
    base_dir = jax.random.normal(key_list[1], (1, D), jnp.float32) * base_size
    mixing = jax.random.uniform(key_list[2], (GROUP, 1), jnp.float32, mix_lo, mix_hi)
    own_shift = jax.random.normal(key_list[3], (GROUP, D), jnp.float32) * own_size
    shard_scale = jax.random.uniform(key_list[4], (GROUP, 1, 1), jnp.float32, scale_lo, scale_hi)
    row_shift = mixing * base_dir + own_shift
    drawn_rows = noise_rows * shard_scale + row_shift[:, None, :]
    return drawn_rows.reshape(TOKENS, D).astype(jnp.bfloat16)


def old_factor(key_one, diag_lo, diag_hi, spread):
    key_pair = jax.random.split(key_one, 2)
    diag_vals = jax.random.uniform(key_pair[0], (LAYERS, D), jnp.float32, diag_lo, diag_hi)
    basis_mat = jax.random.normal(key_pair[1], (LAYERS, D, RANK), jnp.float32) * spread
    low_rank = jnp.einsum("lik,ljk->lij", basis_mat, basis_mat)
    return low_rank + diag_vals[:, :, None] * jnp.eye(D, dtype=jnp.float32)


def inv_factor(key_one, spread):
    key_pair = jax.random.split(key_one, 2)
    raw_draw = jax.random.normal(key_pair[0], (LAYERS, D, D), jnp.float32)
    diag_vals = jax.random.uniform(key_pair[1], (LAYERS, D), jnp.float32, 0.7, 1.5)
    sym_part = (raw_draw + jnp.swapaxes(raw_draw, 1, 2)) * (spread * D ** -0.5)
    return sym_part + diag_vals[:, :, None] * jnp.eye(D, dtype=jnp.float32)


def setup_inputs(seed: int = 0) -> dict:
    key_list = jax.random.split(jax.random.key(seed), 15)
    x_in = sharded_rows(key_list[0:5], 0.8, 0.5, 0.2, 1.0, 0.6, 1.4)
    d_out = sharded_rows(key_list[5:10], 0.6, 0.4, -0.5, 1.0, 0.5, 1.5)
    w_draw = jax.random.normal(key_list[10], (LAYERS, D, D), jnp.float32) * D ** -0.5
    return {"x_in": x_in, "d_out": d_out, "w_stack": w_draw.astype(jnp.bfloat16), "a_old": old_factor(key_list[11], 0.3, 1.2, 0.08), "s_old": old_factor(key_list[12], 0.2, 0.8, 0.06), "a_inv": inv_factor(key_list[13], 0.15), "s_inv": inv_factor(key_list[14], 0.15)}


def reference(x_in, d_out, w_stack, a_old, s_old, a_inv, s_inv):
    layer_in = []
    pre_act = []
    h_cur = x_in
    for layer_idx in range(LAYERS):
        layer_in.append(h_cur)
        z_cur = jnp.dot(h_cur, w_stack[layer_idx], preferred_element_type=jnp.float32).astype(jnp.bfloat16)
        pre_act.append(z_cur)
        if layer_idx < LAYERS - 1:
            h_cur = gelu_fwd(z_cur.astype(jnp.float32)).astype(jnp.bfloat16)
    a_list = []
    s_list = []
    w_list = []
    g_cur = d_out
    for layer_idx in reversed(range(LAYERS)):
        if layer_idx < LAYERS - 1:
            g_cur = (dh_cur.astype(jnp.float32) * gelu_slope(pre_act[layer_idx].astype(jnp.float32))).astype(jnp.bfloat16)
        h_prev = layer_in[layer_idx]
        a_list.append(tok_gram(h_prev, h_prev) / TOKENS)
        s_list.append(tok_gram(g_cur, g_cur) / TOKENS)
        w_list.append(tok_gram(h_prev, g_cur) / TOKENS)
        if layer_idx > 0:
            dh_cur = jnp.dot(g_cur, w_stack[layer_idx].T, preferred_element_type=jnp.float32).astype(jnp.bfloat16)
    a_stack = jnp.stack(a_list[::-1])
    s_stack = jnp.stack(s_list[::-1])
    w_grad = jnp.stack(w_list[::-1])
    left_mul = jnp.einsum("lij,ljk->lik", a_inv, w_grad, precision=lax.Precision.HIGHEST)
    u_stack = jnp.einsum("lij,ljk->lik", left_mul, s_inv, precision=lax.Precision.HIGHEST)
    return (u_stack, RHO * a_old + (1.0 - RHO) * a_stack, RHO * s_old + (1.0 - RHO) * s_stack)
```

```python
import jax
import jax.numpy as jnp
from jax import lax
from jax.sharding import PartitionSpec as P

RHO = 0.75
ERF_SCALE = 0.7071067811865476
PDF_SCALE = 0.3989422804014327
BLK = 128


def tok_gram(lhs_rows, rhs_rows):
    return lax.dot_general(lhs_rows, rhs_rows, (((0,), (0,)), ((), ())), preferred_element_type=jnp.float32)


def times_wt(g_rows, w_mat):
    return lax.dot_general(g_rows, w_mat, (((1,), (1,)), ((), ())), preferred_element_type=jnp.float32)


def gelu_pair(z_val):
    cdf = 0.5 * (1.0 + lax.erf(z_val * ERF_SCALE))
    return z_val * cdf, cdf + z_val * jnp.exp(-0.5 * z_val * z_val) * PDF_SCALE


def pack_halves(top, bot, row0):
    rows, d = top.shape
    half = bot.shape[1]
    r_blk = (row0 + lax.broadcasted_iota(jnp.int32, (rows, d + BLK), 0)) // BLK
    pos = lax.broadcasted_iota(jnp.int32, (rows, d + BLK), 1)
    return jnp.where(pos < BLK * (r_blk + 1), jnp.pad(bot, ((0, 0), (0, d + BLK - half))), jnp.pad(top, ((0, 0), (BLK, 0))))


def sym_gram_packed(rows):
    half = rows.shape[1] // 2
    top = tok_gram(rows[:, :half], rows)
    bot = tok_gram(rows[:, half:], rows[:, half:])
    return pack_halves(top, bot, 0)


def mirror(sq):
    n = sq.shape[0]
    r_blk = lax.broadcasted_iota(jnp.int32, (n, n), 0) // BLK
    c_blk = lax.broadcasted_iota(jnp.int32, (n, n), 1) // BLK
    return r_blk, c_blk


def unpack(packed):
    half = packed.shape[0]
    r_blk = lax.broadcasted_iota(jnp.int32, (half, half), 0) // BLK
    c_blk = lax.broadcasted_iota(jnp.int32, (half, half), 1) // BLK
    tl = packed[:, BLK:BLK + half]
    tr = packed[:, BLK + half:]
    br = packed[:, :half]
    tl = jnp.where(c_blk >= r_blk, tl, tl.T)
    br = jnp.where(c_blk <= r_blk, br, br.T)
    return jnp.concatenate([jnp.concatenate([tl, tr], 1), jnp.concatenate([tr.T, br], 1)], 0)


def hi_dot(lhs, rhs, dims):
    return lax.dot_general(lhs, rhs, (dims, ((), ())), precision=lax.Precision.HIGHEST, preferred_element_type=jnp.float32)


def solution(mesh):
    group_size = mesh.shape["data"]

    def local_step(x_loc, dy_loc, w_stack, a_old, s_old, a_inv, s_inv):
        layers, d = w_stack.shape[0], w_stack.shape[1]
        half = d // 2
        tokens = x_loc.shape[0] * group_size
        me = lax.axis_index("data")
        sh = half // group_size

        def scatter(mats):
            return lax.psum_scatter(jnp.concatenate(mats, 1), "data", scatter_dimension=0, tiled=True)

        def gather(mats):
            return lax.all_gather(jnp.concatenate(mats, 1), "data", axis=0, tiled=True)

        def old_shard(old):
            top = lax.dynamic_slice(old, (me * sh, 0), (sh, d))
            bot = lax.dynamic_slice(old, (half + me * sh, half), (sh, half))
            return pack_halves(top, bot, me * sh)

        pw = d + BLK
        a_fac = [None] * layers
        s_fac = [None] * layers
        w_fac = [None] * layers

        def blend(old, red):
            return RHO * old_shard(old) + (1.0 - RHO) * (red / tokens)

        h_in = [x_loc]
        slope = []
        a_pk = [sym_gram_packed(x_loc)]
        s_pk = [None] * layers
        s_pk[layers - 1] = sym_gram_packed(dy_loc)
        red0 = scatter([a_pk[0], s_pk[layers - 1]])
        for l in range(layers - 1):
            z_cur = jnp.dot(h_in[l], w_stack[l], preferred_element_type=jnp.float32).astype(jnp.bfloat16)
            h_nxt, sl = gelu_pair(z_cur.astype(jnp.float32))
            h_in.append(h_nxt.astype(jnp.bfloat16))
            slope.append(sl)
            a_pk.append(sym_gram_packed(h_in[l + 1]))
        red1 = scatter(a_pk[1:])
        new0 = [blend(a_old[0], red0[:, :pw]), blend(s_old[layers - 1], red0[:, pw:])]
        new1 = [blend(a_old[l], red1[:, (l - 1) * pw:l * pw]) for l in range(1, layers)]
        a_all = gather(new0[:1] + new1 + new0[1:])
        a_new = [unpack(a_all[:, l * pw:(l + 1) * pw]) for l in range(layers)]
        s_new = [None] * layers
        s_new[layers - 1] = unpack(a_all[:, layers * pw:])

        g_cur = dy_loc
        t_loc = [None] * layers
        s_sh = [None] * layers
        for l in reversed(range(layers)):
            if l < layers - 1:
                dh = times_wt(g_cur, w_stack[l + 1]).astype(jnp.bfloat16)
                g_cur = (dh.astype(jnp.float32) * slope[l]).astype(jnp.bfloat16)
            dwt = tok_gram(g_cur, h_in[l])
            mats = [dwt[:half], dwt[half:]]
            if l < layers - 1:
                mats.append(sym_gram_packed(g_cur))
            red = scatter(mats)
            if l < layers - 1:
                s_sh[l] = blend(s_old[l], red[:, 2 * d:])
            rows = jnp.concatenate([red[:, :d], red[:, d:2 * d]], 0) / tokens
            t_loc[l] = hi_dot(a_inv[l], rows, ((1,), (1,)))
        s_all = gather(s_sh[:layers - 1])
        for l in range(layers - 1):
            s_new[l] = unpack(s_all[:, l * pw:(l + 1) * pw])

        t_st = jnp.stack(t_loc, 0)
        q = d // group_size
        t_x = lax.all_to_all(t_st.reshape(layers, group_size, q, 2, sh), "data", split_axis=1, concat_axis=1, tiled=True)
        t_rows = t_x.transpose(0, 2, 3, 1, 4).reshape(layers, q, d)
        u_loc = jnp.stack([hi_dot(t_rows[l], s_inv[l], ((1,), (0,))) for l in range(layers)], 0)
        u_stack = lax.all_gather(u_loc, "data", axis=1, tiled=True)
        return u_stack, jnp.stack(a_new), jnp.stack(s_new)

    row_spec = P("data", None)
    full_spec = P()
    return jax.shard_map(local_step, mesh=mesh, in_specs=(row_spec, row_spec, full_spec, full_spec, full_spec, full_spec, full_spec), out_specs=(full_spec, full_spec, full_spec), check_vma=False)
```

```python
import functools

import jax
import jax.numpy as jnp
from jax import lax
from jax.experimental import pallas as pl
from jax.experimental.pallas import tpu as pltpu
from jax.sharding import PartitionSpec as P

RHO = 0.75
ERF_SCALE = 0.7071067811865476
PDF_SCALE = 0.3989422804014327
D = 1024
B = 256
NT = 8
F32 = jnp.float32
BF16 = jnp.bfloat16

SYM_BLOCKS = [(bi, bj) for bj in range(4) for bi in range(bj + 1)]


def dot_f32(lhs, rhs, dims=((1,), (0,)), precision=None):
    return lax.dot_general(lhs, rhs, (dims, ((), ())), precision=precision, preferred_element_type=F32)


class Unit:
    def __init__(self, name, kind, out, old, layer, slot, hooks, rot):
        self.name, self.kind, self.out, self.old, self.layer, self.slot, self.hooks = name, kind, out, old, layer, slot, hooks
        if kind == "sym":
            sizes = [[4, 3, 3], [3, 4, 3], [3, 3, 4]][rot % 3]
        else:
            sizes = [[256, 384, 384], [384, 256, 384], [384, 384, 256]][rot % 3]
        starts = [0, sizes[0], sizes[0] + sizes[1]]
        self.groups = list(zip(starts, sizes))


UNITS = [
    Unit("s4", "sym", 7, "s", 3, 0, [8, 9, 11, 13, 14, 15, 17, 19, 20], 0),
    Unit("a1", "sym", 0, "a", 0, 1, [8, 10, 12, 14, 15, 16, 18, 20, 21], 1),
    Unit("a2", "sym", 1, "a", 1, 2, [16, 17, 19, 21, 22, 23, 25, 27, 28], 2),
    Unit("a3", "sym", 2, "a", 2, 0, [24, 25, 27, 29, 30, 31, 33, 36, 38], 0),
    Unit("a4", "sym", 3, "a", 3, 1, [32, 34, 37, 40, 41, 42, 43, 44, 45], 1),
    Unit("w4", "full", 3, None, 3, 0, [40, 42, 44, 46, 47, 48, 49, 51, 53], 0),
    Unit("s3", "sym", 6, "s", 2, 2, [48, 49, 51, 52, 53, 54, 55, 57, 58], 2),
    Unit("w3", "full", 2, None, 2, 1, [48, 50, 52, 54, 55, 56, 57, 59, 61], 1),
    Unit("s2", "sym", 5, "s", 1, 0, [56, 57, 59, 60, 61, 62, 63, 65, 66], 0),
    Unit("w2", "full", 1, None, 1, 0, [56, 58, 60, 62, 63, 64, 65, 66, 67], 2),
    Unit("w1", "full", 0, None, 0, 1, [64, 65, 66, 67, 68, 69, 70, 71, 72], 0),
    Unit("s1", "sym", 4, "s", 0, 1, [64, 65, 66, 67, 68, 69, 70, 71, 72], 1),
]


def step_kernel(tm, tokens, x_hbm, dy_hbm, w_hbm, aold_hbm, sold_hbm, ainv_hbm,
                osym, ovt, z_hbm, h_hbm,
                cur, ht, w_buf, st_a, st_b, z_out, ainv_buf,
                sacc, facc, sr0, sr1, sr2, sr3, fr0, fr1, fr2, fr3, old_buf, spc, fpc,
                send_sem, recv_sem, loc_sem, old_sem, x_sem, h_sem, w_sem, sta_sem, stb_sem, z_sem, ainv_sem):
    me = lax.axis_index("data")
    core = lax.rem(me, 2)
    pos = [lax.rem(me // 2, 2), lax.rem(me // 4, 2), lax.rem(me // 8, 2)]
    core_peer = me + 1 - 2 * core
    peers = [me + (1 - 2 * pos[d]) * (2 << d) for d in range(3)]

    sym_recv = [sr0, sr1, sr2, sr3]
    full_recv = [fr0, fr1, fr2, fr3]

    def dims_of(g):
        return [g, (g + 1) % 3, (g + 2) % 3]

    def base_size(u, g):
        return (0, B) if u.kind == "sym" else u.groups[g]

    def offset(u, g, level):
        r0, n = base_size(u, g)
        bits = [core] + [pos[d] for d in dims_of(g)]
        off = r0
        for i in range(level):
            off = off + bits[i] * (n >> (i + 1))
        return pl.multiple_of(off, 8) if level else off

    def other(u, g, level):
        r0, n = base_size(u, g)
        bits = [core] + [pos[d] for d in dims_of(g)]
        return pl.multiple_of(offset(u, g, level) + (1 - bits[level]) * (n >> (level + 1)), 8)

    def peer(g, level):
        return core_peer if level == 0 else peers[dims_of(g)[level - 1]]

    def rows(u, g, level):
        return base_size(u, g)[1] >> level

    def acc_at(u, g, off, size):
        if u.kind == "sym":
            b0, nb = u.groups[g]
            return sacc.at[u.slot, pl.ds(b0, nb), pl.ds(off, size), :]
        return facc.at[u.slot, pl.ds(off, size), :]

    def recv_at(u, g, level):
        if u.kind == "sym":
            b0, nb = u.groups[g]
            return sym_recv[level].at[u.slot, pl.ds(b0, nb)]
        r0, n = u.groups[g]
        return full_recv[level].at[u.slot, pl.ds(r0 >> (level + 1), n >> (level + 1)), :]

    def piece_at(u, g):
        if u.kind == "sym":
            b0, nb = u.groups[g]
            return spc.at[u.slot, pl.ds(b0, nb)]
        r0, n = u.groups[g]
        return fpc.at[u.slot, pl.ds(r0 >> 4, n >> 4), :]

    def out_at(u, g, off, size):
        if u.kind == "sym":
            b0, nb = u.groups[g]
            return osym.at[u.out, pl.ds(b0, nb), pl.ds(off, size), :]
        return ovt.at[u.out, pl.ds(off, size), :]

    def sem_row(u):
        return u.slot if u.kind == "sym" else 3 + u.slot

    def rs_copy(u, g, level):
        return pltpu.make_async_remote_copy(
            src_ref=acc_at(u, g, other(u, g, level), rows(u, g, level + 1)), dst_ref=recv_at(u, g, level),
            send_sem=send_sem.at[sem_row(u), g], recv_sem=recv_sem.at[sem_row(u), level, g],
            device_id=(peer(g, level),), device_id_type=pl.DeviceIdType.MESH)

    def ag_copy(u, g, level):
        off, size = offset(u, g, level + 1), rows(u, g, level + 1)
        src = piece_at(u, g) if level == 3 else out_at(u, g, off, size)
        return pltpu.make_async_remote_copy(
            src_ref=src, dst_ref=out_at(u, g, off, size),
            send_sem=send_sem.at[sem_row(u), g], recv_sem=recv_sem.at[sem_row(u), 7 - level, g],
            device_id=(peer(g, level),), device_id_type=pl.DeviceIdType.MESH)

    def own_copy(u, g):
        return pltpu.make_async_copy(piece_at(u, g), out_at(u, g, offset(u, g, 4), rows(u, g, 4)), loc_sem.at[sem_row(u), g])

    def old_copies(u):
        src = aold_hbm if u.old == "a" else sold_hbm
        for g in range(3):
            b0, nb = u.groups[g]
            for b in range(b0, b0 + nb):
                bi, bj = SYM_BLOCKS[b]
                row = pl.multiple_of(bi * B + offset(u, g, 4), 8)
                pltpu.make_async_copy(src.at[u.layer, pl.ds(row, 16), pl.ds(bj * B, B)], old_buf.at[u.slot, b], old_sem.at[u.slot]).start()

    def ainv_copy(layer):
        return pltpu.make_async_copy(ainv_hbm.at[layer], ainv_buf, ainv_sem)

    def event(u, e):
        if e == 0:
            for g in range(3):
                rs_copy(u, g, 0).start()
            if u.kind == "sym":
                old_copies(u)
            return
        if e <= 4:
            level = e - 1
            for g in range(3):
                rs_copy(u, g, level).wait_recv()
                rs_copy(u, g, level).wait_send()
                if e < 4:
                    mine = acc_at(u, g, offset(u, g, level + 1), rows(u, g, level + 1))
                    mine[...] = mine[...] + recv_at(u, g, level)[...]
                    rs_copy(u, g, level + 1).start()
            if e == 4:
                if u.kind == "sym":
                    pltpu.make_async_copy(osym.at[u.out, :, pl.ds(0, 16), :], old_buf.at[u.slot], old_sem.at[u.slot]).wait()
                for g in range(3):
                    total = acc_at(u, g, offset(u, g, 4), rows(u, g, 4))[...] + recv_at(u, g, 3)[...]
                    if u.kind == "sym":
                        b0, nb = u.groups[g]
                        piece_at(u, g)[...] = RHO * old_buf[u.slot, pl.ds(b0, nb)] + (1.0 - RHO) * (total / tokens)
                    else:
                        piece_at(u, g)[...] = total / tokens
                if u.kind == "full":
                    ainv_copy(u.layer).wait()
                    fpc[u.slot] = dot_f32(fpc[u.slot], ainv_buf[...], precision=lax.Precision.HIGHEST)
                    if u.layer > 0:
                        ainv_copy(u.layer - 1).start()
                for g in range(3):
                    own_copy(u, g).start()
                    ag_copy(u, g, 3).start()
            return
        level = 8 - e
        for g in range(3):
            ag_copy(u, g, level).wait_recv()
            ag_copy(u, g, level).wait_send()
            if e == 5:
                own_copy(u, g).wait()
            if e < 8:
                ag_copy(u, g, level - 1).start()

    by_hook = {}
    for u in UNITS:
        for e, h in enumerate(u.hooks):
            by_hook.setdefault(h, []).append((u, e))

    def hook(index):
        for u, e in by_hook.get(index, []):
            event(u, e)

    def hooks_in_loop(phase, k):
        for i in range(NT):
            if by_hook.get(phase * NT + i):
                @pl.when(k == i)
                def _(i=i):
                    hook(phase * NT + i)

    def tile(k):
        return pl.ds(pl.multiple_of(k * tm, tm), tm)

    def x_copy(k):
        return pltpu.make_async_copy(x_hbm.at[tile(k), :], cur.at[tile(k), :], x_sem.at[k])

    def dy_copy(k, slot):
        return pltpu.make_async_copy(dy_hbm.at[tile(k), :], st_a.at[slot], sta_sem.at[slot])

    def hp_copy(layer, k, slot):
        src = x_hbm.at[tile(k), :] if layer == 0 else h_hbm.at[layer - 1, tile(k), :]
        return pltpu.make_async_copy(src, st_a.at[slot], sta_sem.at[slot])

    def zin_copy(layer, k, slot):
        return pltpu.make_async_copy(z_hbm.at[layer, tile(k), :], st_b.at[slot], stb_sem.at[slot])

    def zout_copy(layer, k, slot):
        return pltpu.make_async_copy(z_out.at[slot], z_hbm.at[layer, tile(k), :], z_sem.at[slot])

    def hout_copy(layer, k):
        return pltpu.make_async_copy(cur.at[tile(k), :], h_hbm.at[layer, tile(k), :], h_sem.at[k])

    def w_copy(layer, slot):
        return pltpu.make_async_copy(w_hbm.at[layer], w_buf.at[slot], w_sem.at[slot])

    def sym_add(slot, rows_t, rows_n):
        for j in range(4):
            part = dot_f32(rows_t[:B * (j + 1)], rows_n[:, B * j:B * (j + 1)]).reshape(j + 1, B, B)
            b0 = j * (j + 1) // 2
            sacc[slot, b0:b0 + j + 1] = sacc[slot, b0:b0 + j + 1] + part

    def full_add(slot, rows_t, read_cols):
        for j in range(4):
            cols = pl.ds(B * j, B)
            facc[slot, :, cols] = facc[slot, :, cols] + dot_f32(rows_t, read_cols(j))

    def loop(body):
        lax.fori_loop(0, NT, lambda k, c: (body(k), c)[1], 0)

    for k in range(NT):
        x_copy(k).start()
    dy_copy(0, 0).start()
    w_copy(0, 0).start()
    w_copy(1, 1).start()

    barrier = pltpu.get_barrier_semaphore()
    for p in [core_peer] + peers:
        pl.semaphore_signal(barrier, inc=1, device_id=(p,), device_id_type=pl.DeviceIdType.MESH)
    pl.semaphore_wait(barrier, 4)

    sacc[0] = jnp.zeros_like(sacc[0])
    sacc[1] = jnp.zeros_like(sacc[1])

    def phase0(k):
        slot = lax.rem(k, 2)

        @pl.when(k + 1 < NT)
        def _():
            dy_copy(k + 1, 1 - slot).start()
        x_copy(k).wait()
        dy_copy(k, slot).wait()
        g = st_a[slot]
        sym_add(0, g.T, g)
        h = cur[tile(k), :]
        sym_add(1, h.T, h)

    loop(phase0)

    for layer in range(3):
        phase = layer + 1
        wslot = layer % 2
        aslot = [2, 0, 1][layer]
        if layer > 0:
            w_copy(layer + 1, 1 - wslot).start()
        sacc[aslot] = jnp.zeros_like(sacc[aslot])
        w_copy(layer, wslot).wait()

        def forward(k, layer=layer, phase=phase, wslot=wslot, aslot=aslot):
            hooks_in_loop(phase, k)
            slot = lax.rem(k, 2)

            @pl.when(k >= 2)
            def _():
                zout_copy(layer, k, slot).wait()
            h = cur[tile(k), :]
            for n in range(4):
                cols = pl.ds(B * n, B)
                z = dot_f32(h, w_buf[wslot, :, cols]).astype(BF16)
                z_out[slot, :, cols] = z
                zf = z.astype(F32)
                ht[:, cols] = (0.5 * zf * (1.0 + lax.erf(zf * ERF_SCALE))).astype(BF16)
            zout_copy(layer, k, slot).start()
            h2 = ht[...]
            sym_add(aslot, h2.T, h2)
            if layer > 0:
                hout_copy(layer - 1, k).wait()
            cur[tile(k), :] = ht[...]
            if layer < 2:
                hout_copy(layer, k).start()
            else:
                @pl.when(k == NT - 1)
                def _():
                    dy_copy(0, 0).start()

        loop(forward)
        zout_copy(layer, 0, 0).wait()
        zout_copy(layer, 1, 1).wait()

    facc[0] = jnp.zeros_like(facc[0])

    def top(k):
        hooks_in_loop(4, k)
        slot = lax.rem(k, 2)

        @pl.when(k + 1 < NT)
        def _():
            dy_copy(k + 1, 1 - slot).start()

        dy_copy(k, slot).wait()

        @pl.when(k == NT - 1)
        def _():
            hp_copy(2, 0, 0).start()
            zin_copy(2, 0, 0).start()

        g = st_a[slot]
        full_add(0, g.T, lambda j: cur[tile(k), pl.ds(B * j, B)])
        cur[tile(k), :] = st_a[slot]

    loop(top)

    for layer in (2, 1, 0):
        phase = 7 - layer
        wslot = [1, 0, 1][layer]
        sslot = [1, 0, 2][layer]
        fslot = [1, 0, 1][layer]
        if layer == 2:
            ainv_copy(3).start()
        if layer == 1:
            w_copy(1, 1).start()
        sacc[sslot] = jnp.zeros_like(sacc[sslot])
        facc[fslot] = jnp.zeros_like(facc[fslot])
        if layer != 1:
            w_copy(layer + 1, wslot).wait()

        def backward(k, layer=layer, phase=phase, wslot=wslot, sslot=sslot, fslot=fslot):
            hooks_in_loop(phase, k)
            slot = lax.rem(k, 2)

            @pl.when(k + 1 < NT)
            def _():
                hp_copy(layer, k + 1, 1 - slot).start()
                zin_copy(layer, k + 1, 1 - slot).start()

            hp_copy(layer, k, slot).wait()
            zin_copy(layer, k, slot).wait()
            if layer > 0:
                @pl.when(k == NT - 1)
                def _():
                    hp_copy(layer - 1, 0, 0).start()
                    zin_copy(layer - 1, 0, 0).start()

            g_up = cur[tile(k), :]
            for n in range(4):
                cols = pl.ds(B * n, B)
                dh = dot_f32(g_up, w_buf[wslot, cols, :], ((1,), (1,))).astype(BF16)
                zf = st_b[slot, :, cols].astype(F32)
                slope = 0.5 * (1.0 + lax.erf(zf * ERF_SCALE)) + zf * jnp.exp(-0.5 * zf * zf) * PDF_SCALE
                ht[:, cols] = (dh.astype(F32) * slope).astype(BF16)
            g = ht[...]
            g_t = g.T
            sym_add(sslot, g_t, g)
            full_add(fslot, g_t, lambda j: st_a[slot, :, pl.ds(B * j, B)])
            cur[tile(k), :] = ht[...]

        loop(backward)

    last = max(max(u.hooks) for u in UNITS)
    for index in range(8 * NT, last + 1):
        hook(index)


def unpack_kernel(in_ref, out_ref):
    for b, (bi, bj) in enumerate(SYM_BLOCKS):
        blk = in_ref[0, b]
        out_ref[0, bi * B:(bi + 1) * B, bj * B:(bj + 1) * B] = blk
        if bi != bj:
            out_ref[0, bj * B:(bj + 1) * B, bi * B:(bi + 1) * B] = blk.T


def unpack(osym, first, count):
    return pl.pallas_call(
        unpack_kernel,
        grid=(count,),
        in_specs=[pl.BlockSpec((1, 10, B, B), lambda i: (first + i, 0, 0, 0))],
        out_specs=pl.BlockSpec((1, D, D), lambda i: (i, 0, 0)),
        out_shape=jax.ShapeDtypeStruct((count, D, D), F32),
        compiler_params=pltpu.CompilerParams(vmem_limit_bytes=32 * 1024 * 1024),
    )(osym)


def solution(mesh):
    group_size = mesh.shape["data"]

    def local_step(x_loc, dy_loc, w_stack, a_old, s_old, a_inv, s_inv):
        n_rows = x_loc.shape[0]
        tm = n_rows // NT
        tokens = n_rows * group_size
        any_spec = pl.BlockSpec(memory_space=pl.ANY)
        vm = pltpu.VMEM
        osym, ovt, _, _ = pl.pallas_call(
            functools.partial(step_kernel, tm, float(tokens)),
            out_shape=(
                jax.ShapeDtypeStruct((8, 10, B, B), F32),
                jax.ShapeDtypeStruct((4, D, D), F32),
                jax.ShapeDtypeStruct((3, n_rows, D), BF16),
                jax.ShapeDtypeStruct((2, n_rows, D), BF16),
            ),
            in_specs=[any_spec] * 6,
            out_specs=(any_spec,) * 4,
            scratch_shapes=[
                vm((n_rows, D), BF16), vm((tm, D), BF16), vm((2, D, D), BF16), vm((2, tm, D), BF16), vm((2, tm, D), BF16),
                vm((2, tm, D), BF16), vm((D, D), F32),
                vm((3, 10, B, B), F32), vm((2, D, D), F32),
                vm((3, 10, 128, B), F32), vm((3, 10, 64, B), F32), vm((3, 10, 32, B), F32), vm((3, 10, 16, B), F32),
                vm((2, 512, D), F32), vm((2, 256, D), F32), vm((2, 128, D), F32), vm((2, 64, D), F32),
                vm((3, 10, 16, B), F32), vm((3, 10, 16, B), F32), vm((2, 64, D), F32),
                pltpu.SemaphoreType.DMA((5, 3)), pltpu.SemaphoreType.DMA((5, 8, 3)), pltpu.SemaphoreType.DMA((5, 3)),
                pltpu.SemaphoreType.DMA((3,)), pltpu.SemaphoreType.DMA((NT,)), pltpu.SemaphoreType.DMA((NT,)),
                pltpu.SemaphoreType.DMA((2,)), pltpu.SemaphoreType.DMA((2,)), pltpu.SemaphoreType.DMA((2,)),
                pltpu.SemaphoreType.DMA((2,)), pltpu.SemaphoreType.DMA,
            ],
            compiler_params=pltpu.CompilerParams(collective_id=0, has_side_effects=True, vmem_limit_bytes=67043328),
            name="step_kernel",
        )(x_loc, dy_loc, w_stack, a_old, s_old, a_inv)
        a_new = unpack(osym, 0, 4)
        s_new = unpack(osym, 4, 4)
        u_stack = jnp.einsum("loi,lon->lin", ovt, s_inv, precision=lax.Precision.HIGHEST, preferred_element_type=F32)
        return u_stack, a_new, s_new

    row_spec = P("data", None)
    full_spec = P()
    return jax.shard_map(local_step, mesh=mesh, in_specs=(row_spec, row_spec, full_spec, full_spec, full_spec, full_spec, full_spec), out_specs=(full_spec, full_spec, full_spec), check_vma=False)
```

```python
import functools

import jax
import jax.numpy as jnp
from jax import lax
from jax.experimental import pallas as pl
from jax.experimental.pallas import tpu as pltpu
from jax.sharding import PartitionSpec as P

RHO = 0.75
ERF_SCALE = 0.7071067811865476
PDF_SCALE = 0.3989422804014327
D = 1024
B = 256
NT = 8
F32 = jnp.float32
BF16 = jnp.bfloat16

SYM_BLOCKS = [(bi, bj) for bj in range(4) for bi in range(bj + 1)]


def dot_f32(lhs, rhs, dims=((1,), (0,)), precision=None):
    return lax.dot_general(lhs, rhs, (dims, ((), ())), precision=precision, preferred_element_type=F32)


class Unit:
    def __init__(self, name, kind, out, old, layer, slot, hooks, rot):
        self.name, self.kind, self.out, self.old, self.layer, self.slot, self.hooks = name, kind, out, old, layer, slot, hooks
        if kind == "sym":
            sizes = [[4, 3, 3], [3, 4, 3], [3, 3, 4]][rot % 3]
        else:
            sizes = [[256, 384, 384], [384, 256, 384], [384, 384, 256]][rot % 3]
        starts = [0, sizes[0], sizes[0] + sizes[1]]
        self.groups = list(zip(starts, sizes))


U_START = 6

UNITS = [
    Unit("a1", "sym", 0, "a", 0, 1, [9, 10, 14, 15, 16, 18, 24, 29, 31], 1),
    Unit("w4", "full", 3, None, 3, 0, [40, 41, 44, 46, 47, 48, 50, 55, 56], 0),
    Unit("a3", "sym", 2, "a", 2, 0, [27, 29, 33, 39, 42, 53, 55, 56, 66], 0),
    Unit("s1", "sym", 4, "s", 0, 1, [66, 67, 72, 75, 76, 80, 82, 84, 89], 1),
    Unit("w3", "full", 2, None, 2, 1, [48, 49, 52, 54, 55, 56, 58, 63, 66], 1),
    Unit("s2", "sym", 5, "s", 1, 0, [70, 73, 75, 77, 79, 80, 82, 85, 89], 0),
    Unit("w1", "full", 0, None, 0, 1, [69, 71, 72, 73, 74, 75, 77, 80, 81], 0),
    Unit("s4", "sym", 7, "s", 3, 0, [8, 9, 12, 14, 15, 17, 20, 24, 26], 0),
    Unit("a2", "sym", 1, "a", 1, 2, [19, 22, 27, 32, 34, 38, 46, 52, 54], 2),
    Unit("a4", "sym", 3, "a", 3, 1, [33, 36, 45, 47, 54, 55, 57, 61, 65], 1),
    Unit("w2", "full", 1, None, 1, 0, [57, 59, 64, 69, 71, 72, 73, 75, 77], 2),
    Unit("s3", "sym", 6, "s", 2, 2, [55, 60, 70, 74, 76, 79, 81, 83, 88], 2),
]


def step_kernel(tm, tokens, x_hbm, dy_hbm, w_hbm, aold_hbm, sold_hbm, ainv_hbm, sinv_hbm,
                osym, ovt, u_hbm, z_hbm, h_hbm,
                cur, ht, w_buf, st_a, st_b, ainv_buf, sinv_buf, vt_buf, u_buf,
                sacc, facc, sr0, sr1, sr2, sr3, fr0, fr1, fr2, fr3, old_buf, spc, fpc,
                send_sem, recv_sem, loc_sem, old_sem, x_sem, h_sem, w_sem, sta_sem, stb_sem, z_sem, ainv_sem, sinv_sem, vt_sem, u_sem):
    z_out = st_b
    me = lax.axis_index("data")
    core = lax.rem(me, 2)
    pos = [lax.rem(me // 2, 2), lax.rem(me // 4, 2), lax.rem(me // 8, 2)]
    core_peer = me + 1 - 2 * core
    peers = [me + (1 - 2 * pos[d]) * (2 << d) for d in range(3)]

    sym_recv = [sr0, sr1, sr2, sr3]
    full_recv = [fr0, fr1, fr2, fr3]

    def dims_of(g):
        return [g, (g + 1) % 3, (g + 2) % 3]

    def base_size(u, g):
        return (0, B) if u.kind == "sym" else u.groups[g]

    def offset(u, g, level):
        r0, n = base_size(u, g)
        bits = [core] + [pos[d] for d in dims_of(g)]
        off = r0
        for i in range(level):
            off = off + bits[i] * (n >> (i + 1))
        return pl.multiple_of(off, 8) if level else off

    def other(u, g, level):
        r0, n = base_size(u, g)
        bits = [core] + [pos[d] for d in dims_of(g)]
        return pl.multiple_of(offset(u, g, level) + (1 - bits[level]) * (n >> (level + 1)), 8)

    def peer(g, level):
        return core_peer if level == 0 else peers[dims_of(g)[level - 1]]

    def rows(u, g, level):
        return base_size(u, g)[1] >> level

    def acc_at(u, g, off, size):
        if u.kind == "sym":
            b0, nb = u.groups[g]
            return sacc.at[u.slot, pl.ds(b0, nb), pl.ds(off, size), :]
        return facc.at[u.slot, pl.ds(off, size), :]

    def recv_at(u, g, level):
        if u.kind == "sym":
            b0, nb = u.groups[g]
            return sym_recv[level].at[u.slot, pl.ds(b0, nb)]
        r0, n = u.groups[g]
        return full_recv[level].at[u.slot, pl.ds(r0 >> (level + 1), n >> (level + 1)), :]

    def piece_at(u, g):
        if u.kind == "sym":
            b0, nb = u.groups[g]
            return spc.at[u.slot, pl.ds(b0, nb)]
        r0, n = u.groups[g]
        return fpc.at[u.slot, pl.ds(r0 >> 4, n >> 4), :]

    def out_at(u, g, off, size):
        if u.kind == "sym":
            b0, nb = u.groups[g]
            return osym.at[u.out, pl.ds(b0, nb), pl.ds(off, size), :]
        return ovt.at[u.out, pl.ds(off, size), :]

    def sem_row(u):
        return u.slot if u.kind == "sym" else 3 + u.slot

    def rs_copy(u, g, level):
        return pltpu.make_async_remote_copy(
            src_ref=acc_at(u, g, other(u, g, level), rows(u, g, level + 1)), dst_ref=recv_at(u, g, level),
            send_sem=send_sem.at[sem_row(u), g], recv_sem=recv_sem.at[sem_row(u), level, g],
            device_id=(peer(g, level),), device_id_type=pl.DeviceIdType.MESH)

    def ag_copy(u, g, level):
        off, size = offset(u, g, level + 1), rows(u, g, level + 1)
        src = piece_at(u, g) if level == 3 else out_at(u, g, off, size)
        return pltpu.make_async_remote_copy(
            src_ref=src, dst_ref=out_at(u, g, off, size),
            send_sem=send_sem.at[sem_row(u), g], recv_sem=recv_sem.at[sem_row(u), 7 - level, g],
            device_id=(peer(g, level),), device_id_type=pl.DeviceIdType.MESH)

    def own_copy(u, g):
        return pltpu.make_async_copy(piece_at(u, g), out_at(u, g, offset(u, g, 4), rows(u, g, 4)), loc_sem.at[sem_row(u), g])

    def old_copies(u):
        src = aold_hbm if u.old == "a" else sold_hbm
        for g in range(3):
            b0, nb = u.groups[g]
            for b in range(b0, b0 + nb):
                bi, bj = SYM_BLOCKS[b]
                row = pl.multiple_of(bi * B + offset(u, g, 4), 8)
                pltpu.make_async_copy(src.at[u.layer, pl.ds(row, 16), pl.ds(bj * B, B)], old_buf.at[u.slot, b], old_sem.at[u.slot]).start()

    def ainv_copy(layer):
        return pltpu.make_async_copy(ainv_hbm.at[layer], ainv_buf, ainv_sem)

    def event(u, e):
        if e == 0:
            for g in range(3):
                rs_copy(u, g, 0).start()
            if u.kind == "sym":
                old_copies(u)
            return
        if e <= 4:
            level = e - 1
            for g in range(3):
                rs_copy(u, g, level).wait_recv()
                rs_copy(u, g, level).wait_send()
                if e < 4:
                    mine = acc_at(u, g, offset(u, g, level + 1), rows(u, g, level + 1))
                    mine[...] = mine[...] + recv_at(u, g, level)[...]
                    rs_copy(u, g, level + 1).start()
            if e == 4:
                if u.kind == "sym":
                    pltpu.make_async_copy(osym.at[u.out, :, pl.ds(0, 16), :], old_buf.at[u.slot], old_sem.at[u.slot]).wait()
                for g in range(3):
                    total = acc_at(u, g, offset(u, g, 4), rows(u, g, 4))[...] + recv_at(u, g, 3)[...]
                    if u.kind == "sym":
                        b0, nb = u.groups[g]
                        piece_at(u, g)[...] = RHO * old_buf[u.slot, pl.ds(b0, nb)] + (1.0 - RHO) * (total / tokens)
                    else:
                        piece_at(u, g)[...] = total / tokens
                if u.kind == "full":
                    ainv_copy(u.layer).wait()
                    fpc[u.slot] = dot_f32(fpc[u.slot], ainv_buf[...], precision=lax.Precision.HIGHEST)
                    if u.layer > 0:
                        ainv_copy(u.layer - 1).start()
                for g in range(3):
                    own_copy(u, g).start()
                    ag_copy(u, g, 3).start()
            return
        level = 8 - e
        for g in range(3):
            ag_copy(u, g, level).wait_recv()
            ag_copy(u, g, level).wait_send()
            if e == 5:
                own_copy(u, g).wait()
            if e < 8:
                ag_copy(u, g, level - 1).start()

    by_hook = {}
    for u in UNITS:
        for e, h in enumerate(u.hooks):
            by_hook.setdefault(h, []).append((u, e))

    def hook(index):
        for u, e in by_hook.get(index, []):
            event(u, e)

    def hooks_in_loop(phase, k):
        for i in range(NT):
            if by_hook.get(phase * NT + i):
                @pl.when(k == i)
                def _(i=i):
                    hook(phase * NT + i)

    def tile(k):
        return pl.ds(pl.multiple_of(k * tm, tm), tm)

    def x_copy(k):
        return pltpu.make_async_copy(x_hbm.at[tile(k), :], cur.at[tile(k), :], x_sem.at[k])

    def dy_copy(k, slot):
        return pltpu.make_async_copy(dy_hbm.at[tile(k), :], st_a.at[slot], sta_sem.at[slot])

    def hp_copy(layer, k, slot):
        src = x_hbm.at[tile(k), :] if layer == 0 else h_hbm.at[layer - 1, tile(k), :]
        return pltpu.make_async_copy(src, st_a.at[slot], sta_sem.at[slot])

    def zin_copy(layer, k, slot):
        return pltpu.make_async_copy(z_hbm.at[layer, tile(k), :], st_b.at[slot], stb_sem.at[slot])

    def zout_copy(layer, k, slot):
        return pltpu.make_async_copy(z_out.at[slot], z_hbm.at[layer, tile(k), :], z_sem.at[slot])

    def hout_copy(layer, k):
        return pltpu.make_async_copy(cur.at[tile(k), :], h_hbm.at[layer, tile(k), :], h_sem.at[k])

    def w_copy(layer, slot):
        return pltpu.make_async_copy(w_hbm.at[layer], w_buf.at[slot], w_sem.at[slot])

    def sym_add(slot, rows_t, rows_n):
        for j in range(4):
            part = dot_f32(rows_t[:B * (j + 1)], rows_n[:, B * j:B * (j + 1)]).reshape(j + 1, B, B)
            b0 = j * (j + 1) // 2
            sacc[slot, b0:b0 + j + 1] = sacc[slot, b0:b0 + j + 1] + part

    def full_add(slot, rows_t, read_cols):
        for j in range(4):
            cols = pl.ds(B * j, B)
            facc[slot, :, cols] = facc[slot, :, cols] + dot_f32(rows_t, read_cols(j))

    def loop(body):
        lax.fori_loop(0, NT, lambda k, c: (body(k), c)[1], 0)

    for k in range(NT):
        x_copy(k).start()
    dy_copy(0, 0).start()
    w_copy(0, 0).start()
    w_copy(1, 1).start()

    barrier = pltpu.get_barrier_semaphore()
    for p in [core_peer] + peers:
        pl.semaphore_signal(barrier, inc=1, device_id=(p,), device_id_type=pl.DeviceIdType.MESH)
    pl.semaphore_wait(barrier, 4)

    sacc[0] = jnp.zeros_like(sacc[0])
    sacc[1] = jnp.zeros_like(sacc[1])

    def phase0(k):
        slot = lax.rem(k, 2)

        @pl.when(k + 1 < NT)
        def _():
            dy_copy(k + 1, 1 - slot).start()
        x_copy(k).wait()
        dy_copy(k, slot).wait()
        g = st_a[slot]
        sym_add(0, g.T, g)
        h = cur[tile(k), :]
        sym_add(1, h.T, h)

    loop(phase0)

    for layer in range(3):
        phase = layer + 1
        wslot = layer % 2
        aslot = [2, 0, 1][layer]
        if layer > 0:
            w_copy(layer + 1, 1 - wslot).start()
        sacc[aslot] = jnp.zeros_like(sacc[aslot])
        w_copy(layer, wslot).wait()

        def forward(k, layer=layer, phase=phase, wslot=wslot, aslot=aslot):
            hooks_in_loop(phase, k)
            slot = lax.rem(k, 2)

            @pl.when(k >= 2)
            def _():
                zout_copy(layer, k, slot).wait()
            h = cur[tile(k), :]
            for n in range(4):
                cols = pl.ds(B * n, B)
                z = dot_f32(h, w_buf[wslot, :, cols]).astype(BF16)
                z_out[slot, :, cols] = z
                zf = z.astype(F32)
                ht[:, cols] = (0.5 * zf * (1.0 + lax.erf(zf * ERF_SCALE))).astype(BF16)
            zout_copy(layer, k, slot).start()
            h2 = ht[...]
            sym_add(aslot, h2.T, h2)
            if layer > 0:
                hout_copy(layer - 1, k).wait()
            cur[tile(k), :] = ht[...]
            if layer < 2:
                hout_copy(layer, k).start()
            else:
                @pl.when(k == NT - 1)
                def _():
                    dy_copy(0, 0).start()

        loop(forward)
        zout_copy(layer, 0, 0).wait()
        zout_copy(layer, 1, 1).wait()

    facc[0] = jnp.zeros_like(facc[0])

    def top(k):
        hooks_in_loop(4, k)
        slot = lax.rem(k, 2)

        @pl.when(k + 1 < NT)
        def _():
            dy_copy(k + 1, 1 - slot).start()

        dy_copy(k, slot).wait()

        @pl.when(k == NT - 1)
        def _():
            hp_copy(2, 0, 0).start()
            zin_copy(2, 0, 0).start()

        g = st_a[slot]
        full_add(0, g.T, lambda j: cur[tile(k), pl.ds(B * j, B)])
        cur[tile(k), :] = st_a[slot]

    loop(top)

    for layer in (2, 1, 0):
        phase = 7 - layer
        wslot = [1, 0, 1][layer]
        sslot = [1, 0, 2][layer]
        fslot = [1, 0, 1][layer]
        if layer == 2:
            ainv_copy(3).start()
        if layer == 1:
            w_copy(1, 1).start()
        sacc[sslot] = jnp.zeros_like(sacc[sslot])
        facc[fslot] = jnp.zeros_like(facc[fslot])
        if layer != 1:
            w_copy(layer + 1, wslot).wait()

        def backward(k, layer=layer, phase=phase, wslot=wslot, sslot=sslot, fslot=fslot):
            hooks_in_loop(phase, k)
            slot = lax.rem(k, 2)

            @pl.when(k + 1 < NT)
            def _():
                hp_copy(layer, k + 1, 1 - slot).start()
                zin_copy(layer, k + 1, 1 - slot).start()

            hp_copy(layer, k, slot).wait()
            zin_copy(layer, k, slot).wait()
            if layer > 0:
                @pl.when(k == NT - 1)
                def _():
                    hp_copy(layer - 1, 0, 0).start()
                    zin_copy(layer - 1, 0, 0).start()

            g_up = cur[tile(k), :]
            for n in range(4):
                cols = pl.ds(B * n, B)
                dh = dot_f32(g_up, w_buf[wslot, cols, :], ((1,), (1,))).astype(BF16)
                zf = st_b[slot, :, cols].astype(F32)
                slope = 0.5 * (1.0 + lax.erf(zf * ERF_SCALE)) + zf * jnp.exp(-0.5 * zf * zf) * PDF_SCALE
                ht[:, cols] = (dh.astype(F32) * slope).astype(BF16)
            g = ht[...]
            g_t = g.T
            sym_add(sslot, g_t, g)
            full_add(fslot, g_t, lambda j: st_a[slot, :, pl.ds(B * j, B)])
            cur[tile(k), :] = ht[...]

        loop(backward)

    last = max(max(u.hooks) for u in UNITS)
    n_last = max(last + 1 - 8 * NT, U_START + 16)

    def sinv_copy(layer):
        return pltpu.make_async_copy(sinv_hbm.at[layer], sinv_buf, sinv_sem)

    def vt_copy(layer, m, slot):
        return pltpu.make_async_copy(ovt.at[layer, :, pl.ds(pl.multiple_of(m * B, B), B)], vt_buf.at[slot], vt_sem.at[slot])

    def u_copy(layer, m):
        return pltpu.make_async_copy(u_buf, u_hbm.at[layer, pl.ds(pl.multiple_of(m * B, B), B), :], u_sem)

    sinv_copy(3).start()

    def final(s, carry):
        for i in range(n_last):
            if by_hook.get(8 * NT + i):
                @pl.when(s == i)
                def _(i=i):
                    hook(8 * NT + i)

        @pl.when((s + 1 >= U_START) & (s + 1 < U_START + 16))
        def _():
            p = s + 1 - U_START
            vt_copy(3 - p // 4, lax.rem(p, 4), lax.rem(p, 2)).start()

        @pl.when((s >= U_START) & (s < U_START + 16))
        def _():
            p = s - U_START
            layer, m, slot = 3 - p // 4, lax.rem(p, 4), lax.rem(p, 2)

            @pl.when(m == 0)
            def _():
                sinv_copy(layer).wait()

            vt_copy(layer, m, slot).wait()

            @pl.when(p > 0)
            def _():
                u_copy(layer, m).wait()
            for j in range(2):
                part = dot_f32(sinv_buf[512 * j:512 * (j + 1), :], vt_buf[slot], precision=lax.Precision.HIGHEST)
                u_buf[:, 512 * j:512 * (j + 1)] = part.T
            u_copy(layer, m).start()

            @pl.when((m == 3) & (layer > 0))
            def _():
                sinv_copy(layer - 1).start()
        return carry

    lax.fori_loop(0, n_last, final, 0)
    u_copy(0, 3).wait()


def tail_kernel(sym_ref, u_ref, u_out, a_out, s_out):
    u_out[...] = u_ref[...]

    def expand(out_ref):
        for b, (bi, bj) in enumerate(SYM_BLOCKS):
            blk = sym_ref[0, b]
            out_ref[0, bi * B:(bi + 1) * B, bj * B:(bj + 1) * B] = blk
            if bi != bj:
                out_ref[0, bj * B:(bj + 1) * B, bi * B:(bi + 1) * B] = blk.T

    @pl.when(pl.program_id(0) < 4)
    def _():
        expand(a_out)

    @pl.when(pl.program_id(0) >= 4)
    def _():
        expand(s_out)


def tail(osym, u_part):
    full = jax.ShapeDtypeStruct((4, D, D), F32)
    return pl.pallas_call(
        tail_kernel,
        grid=(8,),
        in_specs=[pl.BlockSpec((1, 10, B, B), lambda i: (i, 0, 0, 0)), pl.BlockSpec((1, D // 2, D), lambda i: (i // 2, i % 2, 0))],
        out_specs=(pl.BlockSpec((1, D // 2, D), lambda i: (i // 2, i % 2, 0)), pl.BlockSpec((1, D, D), lambda i: (jnp.minimum(i, 3), 0, 0)), pl.BlockSpec((1, D, D), lambda i: (jnp.maximum(i - 4, 0), 0, 0))),
        out_shape=(full, full, full),
        compiler_params=pltpu.CompilerParams(vmem_limit_bytes=48 * 1024 * 1024),
        name="tail_kernel",
    )(osym, u_part)


def solution(mesh):
    group_size = mesh.shape["data"]

    def local_step(x_loc, dy_loc, w_stack, a_old, s_old, a_inv, s_inv):
        n_rows = x_loc.shape[0]
        tm = n_rows // NT
        tokens = n_rows * group_size
        any_spec = pl.BlockSpec(memory_space=pl.ANY)
        vm = pltpu.VMEM
        osym, _, u_part, _, _ = pl.pallas_call(
            functools.partial(step_kernel, tm, float(tokens)),
            out_shape=(
                jax.ShapeDtypeStruct((8, 10, B, B), F32),
                jax.ShapeDtypeStruct((4, D, D), F32),
                jax.ShapeDtypeStruct((4, D, D), F32),
                jax.ShapeDtypeStruct((3, n_rows, D), BF16),
                jax.ShapeDtypeStruct((2, n_rows, D), BF16),
            ),
            in_specs=[any_spec] * 7,
            out_specs=(any_spec,) * 5,
            scratch_shapes=[
                vm((n_rows, D), BF16), vm((tm, D), BF16), vm((2, D, D), BF16), vm((2, tm, D), BF16), vm((2, tm, D), BF16),
                vm((D, D), F32), vm((D, D), F32), vm((2, D, B), F32), vm((B, D), F32),
                vm((3, 10, B, B), F32), vm((2, D, D), F32),
                vm((3, 10, 128, B), F32), vm((3, 10, 64, B), F32), vm((3, 10, 32, B), F32), vm((3, 10, 16, B), F32),
                vm((2, 512, D), F32), vm((2, 256, D), F32), vm((2, 128, D), F32), vm((2, 64, D), F32),
                vm((3, 10, 16, B), F32), vm((3, 10, 16, B), F32), vm((2, 64, D), F32),
                pltpu.SemaphoreType.DMA((5, 3)), pltpu.SemaphoreType.DMA((5, 8, 3)), pltpu.SemaphoreType.DMA((5, 3)),
                pltpu.SemaphoreType.DMA((3,)), pltpu.SemaphoreType.DMA((NT,)), pltpu.SemaphoreType.DMA((NT,)),
                pltpu.SemaphoreType.DMA((2,)), pltpu.SemaphoreType.DMA((2,)), pltpu.SemaphoreType.DMA((2,)),
                pltpu.SemaphoreType.DMA((2,)), pltpu.SemaphoreType.DMA, pltpu.SemaphoreType.DMA, pltpu.SemaphoreType.DMA((2,)), pltpu.SemaphoreType.DMA,
            ],
            compiler_params=pltpu.CompilerParams(collective_id=0, has_side_effects=True, vmem_limit_bytes=67043328),
            name="step_kernel",
        )(x_loc, dy_loc, w_stack, a_old, s_old, a_inv, s_inv)
        return tail(osym, u_part)

    row_spec = P("data", None)
    full_spec = P()
    return jax.shard_map(local_step, mesh=mesh, in_specs=(row_spec, row_spec, full_spec, full_spec, full_spec, full_spec, full_spec), out_specs=(full_spec, full_spec, full_spec), check_vma=False)
```

```python
import functools

import jax
import jax.numpy as jnp
from jax import lax
from jax.experimental import pallas as pl
from jax.experimental.pallas import tpu as pltpu
from jax.sharding import PartitionSpec as P

RHO = 0.75
ERF_SCALE = 0.7071067811865476
PDF_SCALE = 0.3989422804014327
D = 1024
B = 256
NT = 8
F32 = jnp.float32
BF16 = jnp.bfloat16

SYM_BLOCKS = [(bi, bj) for bj in range(4) for bi in range(bj + 1)]
NB = len(SYM_BLOCKS) - 1
Q = B // 2
DIAG = [SYM_BLOCKS.index((i, i)) for i in range(4)]
CARRIED = [(0, 0), (0, 1), (1, 1)]


def dot_f32(lhs, rhs, dims=((1,), (0,)), precision=None):
    return lax.dot_general(lhs, rhs, (dims, ((), ())), precision=precision, preferred_element_type=F32)


class Unit:
    def __init__(self, kind, layer, slot, first, gaps, rot):
        self.kind, self.old, self.layer, self.slot = ("full" if kind == "w" else "sym"), kind, layer, slot
        self.out = layer + (4 if kind == "s" else 0)
        self.hooks = [first]
        for gap in gaps:
            self.hooks.append(self.hooks[-1] + int(gap))
        if self.kind == "sym":
            sizes = [3, 3, 3]
        else:
            sizes = [384, 384, 384]
            sizes[rot % 3] = 256
        starts = [0, sizes[0], sizes[0] + sizes[1]]
        self.groups = list(zip(starts, sizes))


U_PIECES = 8
U_START = 13

UNITS = [
    Unit("s", 0, 1, 77, "22214224", 0),
    Unit("w", 1, 0, 67, "28321131", 2),
    Unit("a", 3, 1, 42, "76223118", 0),
    Unit("w", 2, 1, 56, "23111246", 1),
    Unit("a", 1, 2, 28, "24522365", 0),
    Unit("w", 3, 0, 48, "23111244", 0),
    Unit("s", 1, 0, 65, "37713328", 0),
    Unit("a", 2, 0, 34, "27542130", 0),
    Unit("a", 0, 1, 17, "63223233", 0),
    Unit("w", 0, 1, 77, "31111321", 0),
    Unit("s", 2, 2, 61, "37734322", 0),
    Unit("s", 3, 0, 8, "83213233", 0),
]


def step_kernel(tm, tokens, x_hbm, dy_hbm, w_hbm, aold_hbm, sold_hbm, ainv_hbm, sinv_hbm,
                osym, ovt, u_hbm, z_hbm, h_hbm,
                cur, ht, w_buf, st_a, st_b, ainv_buf, sinv_buf, vt_buf, u_buf,
                sacc, facc, sr0, sr1, sr2, sr3, fr0, fr1, fr2, fr3, old_buf, spc, fpc,
                send_sem, recv_sem, loc_sem, old_sem, x_sem, h_sem, w_sem, sta_sem, stb_sem, z_sem, ainv_sem, sinv_sem, vt_sem, u_sem, u_send_sem, u_recv_sem):
    z_out = st_b
    me = lax.axis_index("data")
    core = lax.rem(me, 2)
    pos = [lax.rem(me // 2, 2), lax.rem(me // 4, 2), lax.rem(me // 8, 2)]
    core_peer = me + 1 - 2 * core
    peers = [me + (1 - 2 * pos[d]) * (2 << d) for d in range(3)]

    sym_recv = [sr0, sr1, sr2, sr3]
    full_recv = [fr0, fr1, fr2, fr3]

    def dims_of(g):
        return [g, (g + 1) % 3, (g + 2) % 3]

    def base_size(u, g):
        return (0, B) if u.kind == "sym" else u.groups[g]

    def offset(u, g, level):
        r0, n = base_size(u, g)
        bits = [core] + [pos[d] for d in dims_of(g)]
        off = r0
        for i in range(level):
            off = off + bits[i] * (n >> (i + 1))
        return pl.multiple_of(off, 8) if level else off

    def other(u, g, level):
        r0, n = base_size(u, g)
        bits = [core] + [pos[d] for d in dims_of(g)]
        return pl.multiple_of(offset(u, g, level) + (1 - bits[level]) * (n >> (level + 1)), 8)

    def peer(g, level):
        return core_peer if level == 0 else peers[dims_of(g)[level - 1]]

    def rows(u, g, level):
        return base_size(u, g)[1] >> level

    def acc_at(u, g, off, size):
        if u.kind == "sym":
            b0, nb = u.groups[g]
            return sacc.at[u.slot, pl.ds(b0, nb), pl.ds(off, size), :]
        return facc.at[u.slot, pl.ds(off, size), :]

    def recv_at(u, g, level):
        if u.kind == "sym":
            b0, nb = u.groups[g]
            return sym_recv[level].at[u.slot, pl.ds(b0, nb)]
        r0, n = u.groups[g]
        return full_recv[level].at[u.slot, pl.ds(r0 >> (level + 1), n >> (level + 1)), :]

    def piece_at(u, g):
        if u.kind == "sym":
            b0, nb = u.groups[g]
            return spc.at[u.slot, pl.ds(b0, nb)]
        r0, n = u.groups[g]
        return fpc.at[u.slot, pl.ds(r0 >> 4, n >> 4), :]

    def out_at(u, g, off, size):
        if u.kind == "sym":
            b0, nb = u.groups[g]
            return osym.at[u.out, pl.ds(b0, nb), pl.ds(off, size), :]
        return ovt.at[u.out, pl.ds(off, size), :]

    def sem_row(u):
        return u.slot if u.kind == "sym" else 3 + u.slot

    def rs_copy(u, g, level):
        return pltpu.make_async_remote_copy(
            src_ref=acc_at(u, g, other(u, g, level), rows(u, g, level + 1)), dst_ref=recv_at(u, g, level),
            send_sem=send_sem.at[sem_row(u), g], recv_sem=recv_sem.at[sem_row(u), level, g],
            device_id=(peer(g, level),), device_id_type=pl.DeviceIdType.MESH)

    def ag_copy(u, g, level):
        off, size = offset(u, g, level + 1), rows(u, g, level + 1)
        src = piece_at(u, g) if level == 3 else out_at(u, g, off, size)
        return pltpu.make_async_remote_copy(
            src_ref=src, dst_ref=out_at(u, g, off, size),
            send_sem=send_sem.at[sem_row(u), g], recv_sem=recv_sem.at[sem_row(u), 7 - level, g],
            device_id=(peer(g, level),), device_id_type=pl.DeviceIdType.MESH)

    def own_copy(u, g):
        return pltpu.make_async_copy(piece_at(u, g), out_at(u, g, offset(u, g, 4), rows(u, g, 4)), loc_sem.at[sem_row(u), g])

    def old_copies(u):
        src = aold_hbm if u.old == "a" else sold_hbm
        for g in range(3):
            b0, nb = u.groups[g]
            for b in range(b0, b0 + nb):
                bi, bj = SYM_BLOCKS[b]
                row = pl.multiple_of(bi * B + offset(u, g, 4), 8)
                for half in range(2):
                    from_row, from_col = row, bj * B + half * Q
                    if bi == bj and half == 0:
                        c_row, c_col = CARRIED[bi]
                        from_row = pl.multiple_of(row + core * ((3 - bi) * B - Q + c_row * Q), 8)
                        from_col = pl.multiple_of(from_col + core * ((3 - bi) * B + c_col * Q), Q)
                    pltpu.make_async_copy(src.at[u.layer, pl.ds(from_row, 16), pl.ds(from_col, Q)], old_buf.at[u.slot, b, :, pl.ds(half * Q, Q)], old_sem.at[u.slot]).start()

    def ainv_copy(layer):
        return pltpu.make_async_copy(ainv_hbm.at[layer], ainv_buf, ainv_sem)

    def event(u, e):
        if e == 0:
            if u.kind == "sym":
                for i, (c_row, c_col) in enumerate(CARRIED):
                    sacc[u.slot, DIAG[i], Q:, :Q] = sacc[u.slot, NB, c_row * Q:(c_row + 1) * Q, c_col * Q:(c_col + 1) * Q]
            for g in range(3):
                rs_copy(u, g, 0).start()
            if u.kind == "sym":
                old_copies(u)
            return
        if e <= 4:
            level = e - 1
            for g in range(3):
                rs_copy(u, g, level).wait_recv()
                rs_copy(u, g, level).wait_send()
                if e < 4:
                    mine = acc_at(u, g, offset(u, g, level + 1), rows(u, g, level + 1))
                    mine[...] = mine[...] + recv_at(u, g, level)[...]
                    rs_copy(u, g, level + 1).start()
            if e == 4:
                if u.kind == "sym":
                    pltpu.make_async_copy(osym.at[u.out, :, pl.ds(0, 16), :], old_buf.at[u.slot], old_sem.at[u.slot]).wait()
                for g in range(3):
                    total = acc_at(u, g, offset(u, g, 4), rows(u, g, 4))[...] + recv_at(u, g, 3)[...]
                    if u.kind == "sym":
                        b0, nb = u.groups[g]
                        piece_at(u, g)[...] = RHO * old_buf[u.slot, pl.ds(b0, nb)] + (1.0 - RHO) * (total / tokens)
                    else:
                        piece_at(u, g)[...] = total / tokens
                if u.kind == "full":
                    ainv_copy(u.layer).wait()
                    fpc[u.slot] = dot_f32(fpc[u.slot], ainv_buf[...], precision=lax.Precision.HIGHEST)
                    if u.layer > 0:
                        ainv_copy(u.layer - 1).start()
                for g in range(3):
                    own_copy(u, g).start()
                    ag_copy(u, g, 3).start()
            return
        level = 8 - e
        for g in range(3):
            ag_copy(u, g, level).wait_recv()
            ag_copy(u, g, level).wait_send()
            if e == 5:
                own_copy(u, g).wait()
            if e < 8:
                ag_copy(u, g, level - 1).start()

    by_hook = {}
    for u in UNITS:
        for e, h in enumerate(u.hooks):
            by_hook.setdefault(h, []).append((u, e))

    def hook(index):
        for u, e in by_hook.get(index, []):
            event(u, e)

    def hooks_in_loop(phase, k):
        for i in range(NT):
            if by_hook.get(phase * NT + i):
                @pl.when(k == i)
                def _(i=i):
                    hook(phase * NT + i)

    def tile(k):
        return pl.ds(pl.multiple_of(k * tm, tm), tm)

    def x_copy(k):
        return pltpu.make_async_copy(x_hbm.at[tile(k), :], cur.at[tile(k), :], x_sem.at[k])

    def dy_copy(k, slot):
        return pltpu.make_async_copy(dy_hbm.at[tile(k), :], st_a.at[slot], sta_sem.at[slot])

    def hp_copy(layer, k, slot):
        src = x_hbm.at[tile(k), :] if layer == 0 else h_hbm.at[layer - 1, tile(k), :]
        return pltpu.make_async_copy(src, st_a.at[slot], sta_sem.at[slot])

    def zin_copy(layer, k, slot):
        return pltpu.make_async_copy(z_hbm.at[layer, tile(k), :], st_b.at[slot], stb_sem.at[slot])

    def zout_copy(layer, k, slot):
        return pltpu.make_async_copy(z_out.at[slot], z_hbm.at[layer, tile(k), :], z_sem.at[slot])

    def hout_copy(layer, k):
        return pltpu.make_async_copy(cur.at[tile(k), :], h_hbm.at[layer, tile(k), :], h_sem.at[k])

    def w_copy(layer, slot):
        return pltpu.make_async_copy(w_hbm.at[layer], w_buf.at[slot], w_sem.at[slot])

    def sym_add(slot, rows_t, rows_n):
        for j in range(4):
            part = dot_f32(rows_t[:B * (j + 1)], rows_n[:, B * j:B * (j + 1)]).reshape(j + 1, B, B)
            b0 = j * (j + 1) // 2
            sacc[slot, b0:b0 + j + 1] = sacc[slot, b0:b0 + j + 1] + part

    def full_add(slot, rows_t, read_cols):
        for j in range(4):
            cols = pl.ds(B * j, B)
            facc[slot, :, cols] = facc[slot, :, cols] + dot_f32(rows_t, read_cols(j))

    def loop(body):
        lax.fori_loop(0, NT, lambda k, c: (body(k), c)[1], 0)

    for k in range(NT):
        x_copy(k).start()
    dy_copy(0, 0).start()
    w_copy(0, 0).start()
    w_copy(1, 1).start()

    barrier = pltpu.get_barrier_semaphore()
    for p in [core_peer] + peers:
        pl.semaphore_signal(barrier, inc=1, device_id=(p,), device_id_type=pl.DeviceIdType.MESH)
    pl.semaphore_wait(barrier, 4)

    sacc[0] = jnp.zeros_like(sacc[0])
    sacc[1] = jnp.zeros_like(sacc[1])

    def gram_dy(k):
        slot = lax.rem(k, 2)

        @pl.when(k + 1 < NT)
        def _():
            dy_copy(k + 1, 1 - slot).start()
        dy_copy(k, slot).wait()
        g = st_a[slot]
        sym_add(0, g.T, g)

    loop(gram_dy)

    def gram_x(k):
        hooks_in_loop(1, k)
        x_copy(k).wait()
        h = cur[tile(k), :]
        sym_add(1, h.T, h)

    loop(gram_x)

    for layer in range(3):
        phase = layer + 2
        wslot = layer % 2
        aslot = [2, 0, 1][layer]
        if layer > 0:
            w_copy(layer + 1, 1 - wslot).start()
        sacc[aslot] = jnp.zeros_like(sacc[aslot])
        w_copy(layer, wslot).wait()

        def forward(k, layer=layer, phase=phase, wslot=wslot, aslot=aslot):
            hooks_in_loop(phase, k)
            slot = lax.rem(k, 2)

            @pl.when(k >= 2)
            def _():
                zout_copy(layer, k, slot).wait()
            h = cur[tile(k), :]
            for n in range(4):
                cols = pl.ds(B * n, B)
                z = dot_f32(h, w_buf[wslot, :, cols]).astype(BF16)
                z_out[slot, :, cols] = z
                zf = z.astype(F32)
                ht[:, cols] = (0.5 * zf * (1.0 + lax.erf(zf * ERF_SCALE))).astype(BF16)
            zout_copy(layer, k, slot).start()
            h2 = ht[...]
            sym_add(aslot, h2.T, h2)
            if layer > 0:
                hout_copy(layer - 1, k).wait()
            cur[tile(k), :] = ht[...]
            if layer < 2:
                hout_copy(layer, k).start()
            else:
                @pl.when(k == NT - 1)
                def _():
                    dy_copy(0, 0).start()

        loop(forward)
        zout_copy(layer, 0, 0).wait()
        zout_copy(layer, 1, 1).wait()

    facc[0] = jnp.zeros_like(facc[0])

    def top(k):
        hooks_in_loop(5, k)
        slot = lax.rem(k, 2)

        @pl.when(k + 1 < NT)
        def _():
            dy_copy(k + 1, 1 - slot).start()

        dy_copy(k, slot).wait()

        @pl.when(k == NT - 1)
        def _():
            hp_copy(2, 0, 0).start()
            zin_copy(2, 0, 0).start()

        g = st_a[slot]
        full_add(0, g.T, lambda j: cur[tile(k), pl.ds(B * j, B)])
        cur[tile(k), :] = st_a[slot]

    loop(top)

    for layer in (2, 1, 0):
        phase = 8 - layer
        wslot = [1, 0, 1][layer]
        sslot = [1, 0, 2][layer]
        fslot = [1, 0, 1][layer]
        if layer == 2:
            ainv_copy(3).start()
        if layer == 1:
            w_copy(1, 1).start()
        sacc[sslot] = jnp.zeros_like(sacc[sslot])
        facc[fslot] = jnp.zeros_like(facc[fslot])
        if layer != 1:
            w_copy(layer + 1, wslot).wait()

        def backward(k, layer=layer, phase=phase, wslot=wslot, sslot=sslot, fslot=fslot):
            hooks_in_loop(phase, k)
            slot = lax.rem(k, 2)

            @pl.when(k + 1 < NT)
            def _():
                hp_copy(layer, k + 1, 1 - slot).start()
                zin_copy(layer, k + 1, 1 - slot).start()

            hp_copy(layer, k, slot).wait()
            zin_copy(layer, k, slot).wait()
            if layer > 0:
                @pl.when(k == NT - 1)
                def _():
                    hp_copy(layer - 1, 0, 0).start()
                    zin_copy(layer - 1, 0, 0).start()

            g_up = cur[tile(k), :]
            for n in range(4):
                cols = pl.ds(B * n, B)
                dh = dot_f32(g_up, w_buf[wslot, cols, :], ((1,), (1,))).astype(BF16)
                zf = st_b[slot, :, cols].astype(F32)
                slope = 0.5 * (1.0 + lax.erf(zf * ERF_SCALE)) + zf * jnp.exp(-0.5 * zf * zf) * PDF_SCALE
                ht[:, cols] = (dh.astype(F32) * slope).astype(BF16)
            g = ht[...]
            g_t = g.T
            sym_add(sslot, g_t, g)
            full_add(fslot, g_t, lambda j: st_a[slot, :, pl.ds(B * j, B)])
            cur[tile(k), :] = ht[...]

        loop(backward)

    first_last = 9 * NT
    n_last = max(max(max(u.hooks) for u in UNITS) + 1 - first_last, U_START + U_PIECES)

    def sinv_copy(layer):
        return pltpu.make_async_copy(sinv_hbm.at[layer], sinv_buf, sinv_sem)

    def vt_copy(layer, m, slot):
        return pltpu.make_async_copy(ovt.at[layer, :, pl.ds(pl.multiple_of(m * B, B), B)], vt_buf.at[slot], vt_sem.at[slot])

    def piece_of(p):
        return 3 - p // 2, 2 * lax.rem(p, 2) + core, lax.rem(p, 2)

    def u_at(layer, m):
        return u_hbm.at[layer, pl.ds(pl.multiple_of(m * B, B), B), :]

    def u_copy(layer, m):
        return pltpu.make_async_copy(u_buf, u_at(layer, m), u_sem)

    def u_send(layer, m, p):
        return pltpu.make_async_remote_copy(
            src_ref=u_buf, dst_ref=u_at(layer, m), send_sem=u_send_sem, recv_sem=u_recv_sem.at[p],
            device_id=(core_peer,), device_id_type=pl.DeviceIdType.MESH)

    sinv_copy(3).start()

    def final(s, carry):
        for i in range(n_last):
            if by_hook.get(first_last + i):
                @pl.when(s == i)
                def _(i=i):
                    hook(first_last + i)

        @pl.when((s + 1 >= U_START) & (s + 1 < U_START + U_PIECES))
        def _():
            vt_copy(*piece_of(s + 1 - U_START)).start()

        @pl.when((s >= U_START) & (s < U_START + U_PIECES))
        def _():
            p = s - U_START
            layer, m, slot = piece_of(p)

            @pl.when(slot == 0)
            def _():
                sinv_copy(layer).wait()

            vt_copy(layer, m, slot).wait()

            @pl.when(p > 0)
            def _():
                u_copy(layer, m).wait()
                u_send(layer, m, p).wait_send()
            for j in range(2):
                part = dot_f32(sinv_buf[512 * j:512 * (j + 1), :], vt_buf[slot], precision=lax.Precision.HIGHEST)
                u_buf[:, 512 * j:512 * (j + 1)] = part.T
            u_copy(layer, m).start()
            u_send(layer, m, p).start()

            @pl.when((slot == 1) & (layer > 0))
            def _():
                sinv_copy(layer - 1).start()
        return carry

    lax.fori_loop(0, n_last, final, 0)
    u_copy(0, core).wait()
    u_send(0, core, 0).wait_send()
    for p in range(U_PIECES):
        layer, m, _ = piece_of(p)
        u_send(layer, m, p).wait_recv()


def tail_kernel(sym_ref, u_ref, u_out, a_out, s_out):
    u_out[...] = u_ref[...]

    def put(out_ref, row, col, blk):
        out_ref[0, row:row + blk.shape[0], col:col + blk.shape[1]] = blk

    def expand(out_ref):
        for b, (bi, bj) in enumerate(SYM_BLOCKS[:NB]):
            row, col = bi * B, bj * B
            if bi != bj:
                put(out_ref, row, col, sym_ref[0, b])
                put(out_ref, col, row, sym_ref[0, b].T)
            else:
                put(out_ref, row, col, sym_ref[0, b, :Q, :])
                put(out_ref, row + Q, col + Q, sym_ref[0, b, Q:, Q:])
                put(out_ref, row + Q, col, sym_ref[0, b, :Q, Q:].T)
                carried = sym_ref[0, b, Q:, :Q]
                c_row, c_col = CARRIED[bi]
                put(out_ref, 3 * B + c_row * Q, 3 * B + c_col * Q, carried)
                if c_row != c_col:
                    put(out_ref, 3 * B + c_col * Q, 3 * B + c_row * Q, carried.T)

    @pl.when(pl.program_id(0) < 4)
    def _():
        expand(a_out)

    @pl.when(pl.program_id(0) >= 4)
    def _():
        expand(s_out)


def tail(osym, u_part):
    full = jax.ShapeDtypeStruct((4, D, D), F32)
    return pl.pallas_call(
        tail_kernel,
        grid=(8,),
        in_specs=[pl.BlockSpec((1, NB, B, B), lambda i: (i, 0, 0, 0)), pl.BlockSpec((1, D // 2, D), lambda i: (i // 2, i % 2, 0))],
        out_specs=(pl.BlockSpec((1, D // 2, D), lambda i: (i // 2, i % 2, 0)), pl.BlockSpec((1, D, D), lambda i: (jnp.minimum(i, 3), 0, 0)), pl.BlockSpec((1, D, D), lambda i: (jnp.maximum(i - 4, 0), 0, 0))),
        out_shape=(full, full, full),
        compiler_params=pltpu.CompilerParams(vmem_limit_bytes=48 * 1024 * 1024),
        name="tail_kernel",
    )(osym, u_part)


def solution(mesh):
    group_size = mesh.shape["data"]

    def local_step(x_loc, dy_loc, w_stack, a_old, s_old, a_inv, s_inv):
        n_rows = x_loc.shape[0]
        tm = n_rows // NT
        tokens = n_rows * group_size
        any_spec = pl.BlockSpec(memory_space=pl.ANY)
        vm = pltpu.VMEM
        osym, _, u_part, _, _ = pl.pallas_call(
            functools.partial(step_kernel, tm, float(tokens)),
            out_shape=(
                jax.ShapeDtypeStruct((8, NB, B, B), F32),
                jax.ShapeDtypeStruct((4, D, D), F32),
                jax.ShapeDtypeStruct((4, D, D), F32),
                jax.ShapeDtypeStruct((3, n_rows, D), BF16),
                jax.ShapeDtypeStruct((2, n_rows, D), BF16),
            ),
            in_specs=[any_spec] * 7,
            out_specs=(any_spec,) * 5,
            scratch_shapes=[
                vm((n_rows, D), BF16), vm((tm, D), BF16), vm((2, D, D), BF16), vm((2, tm, D), BF16), vm((2, tm, D), BF16),
                vm((D, D), F32), vm((D, D), F32), vm((2, D, B), F32), vm((B, D), F32),
                vm((3, NB + 1, B, B), F32), vm((2, D, D), F32),
                *[vm((3, NB, B >> i, B), F32) for i in range(1, 5)],
                *[vm((2, D >> i, D), F32) for i in range(1, 5)],
                vm((3, NB, 16, B), F32), vm((3, NB, 16, B), F32), vm((2, 64, D), F32),
                pltpu.SemaphoreType.DMA((5, 3)), pltpu.SemaphoreType.DMA((5, 8, 3)), pltpu.SemaphoreType.DMA((5, 3)),
                pltpu.SemaphoreType.DMA((3,)), pltpu.SemaphoreType.DMA((NT,)), pltpu.SemaphoreType.DMA((NT,)),
                pltpu.SemaphoreType.DMA((2,)), pltpu.SemaphoreType.DMA((2,)), pltpu.SemaphoreType.DMA((2,)),
                pltpu.SemaphoreType.DMA((2,)), pltpu.SemaphoreType.DMA, pltpu.SemaphoreType.DMA, pltpu.SemaphoreType.DMA((2,)), pltpu.SemaphoreType.DMA,
                pltpu.SemaphoreType.DMA, pltpu.SemaphoreType.DMA((U_PIECES,)),
            ],
            compiler_params=pltpu.CompilerParams(collective_id=0, has_side_effects=True, vmem_limit_bytes=67043328),
            name="step_kernel",
        )(x_loc, dy_loc, w_stack, a_old, s_old, a_inv, s_inv)
        return tail(osym, u_part)

    row_spec = P("data", None)
    full_spec = P()
    return jax.shard_map(local_step, mesh=mesh, in_specs=(row_spec, row_spec, full_spec, full_spec, full_spec, full_spec, full_spec), out_specs=(full_spec, full_spec, full_spec), check_vma=False)
```

```python
import functools

import jax
import jax.numpy as jnp
from jax import lax
from jax.experimental import pallas as pl
from jax.experimental.pallas import tpu as pltpu
from jax.sharding import PartitionSpec as P

RHO = 0.75
ERF_SCALE = 0.7071067811865476
PDF_SCALE = 0.3989422804014327
D = 1024
B = 256
NT = 8
F32 = jnp.float32
BF16 = jnp.bfloat16

SYM_BLOCKS = [(bi, bj) for bj in range(4) for bi in range(bj + 1)]
NB = len(SYM_BLOCKS) - 1
Q = B // 2
DIAG = [SYM_BLOCKS.index((i, i)) for i in range(4)]
CARRIED = [(0, 0), (0, 1), (1, 1)]


def dot_f32(lhs, rhs, dims=((1,), (0,)), precision=None):
    return lax.dot_general(lhs, rhs, (dims, ((), ())), precision=precision, preferred_element_type=F32)


class Unit:
    def __init__(self, kind, layer, slot, first, gaps, rot):
        self.kind, self.old, self.layer, self.slot = ("full" if kind == "w" else "sym"), kind, layer, slot
        self.out = layer + (4 if kind == "s" else 0)
        self.hooks = [first]
        for gap in gaps:
            self.hooks.append(self.hooks[-1] + int(gap))
        if self.kind == "sym":
            sizes = [3, 3, 3]
        else:
            sizes = [384, 384, 384]
            sizes[rot % 3] = 256
        starts = [0, sizes[0], sizes[0] + sizes[1]]
        self.groups = list(zip(starts, sizes))


U_PIECES = 8
U_START = 22

UNITS = [
    Unit("s", 3, 0, 9, "35421232", 0),
    Unit("a", 1, 2, 26, "74222784", 0),
    Unit("a", 3, 1, 42, "46315283", 0),
    Unit("w", 3, 0, 48, "03311151", 0),
    Unit("s", 1, 0, 67, "08993561", 0),
    Unit("a", 0, 1, 16, "14222462", 0),
    Unit("a", 2, 0, 34, "13223984", 0),
    Unit("s", 0, 1, 79, "53542257", 0),
    Unit("w", 0, 1, 76, "16174220", 0),
    Unit("w", 1, 0, 64, "12782571", 2),
    Unit("w", 2, 1, 56, "03311143", 1),
    Unit("s", 2, 2, 68, "08579225", 0),
]


def step_kernel(tm, tokens, x_hbm, dy_hbm, w_hbm, aold_hbm, sold_hbm, ainv_hbm, sinv_hbm,
                osym, ovt, u_hbm, z_hbm, h_hbm,
                cur, ht, w_buf, st_a, st_b, ainv_buf, sinv_buf, vt_buf, u_buf,
                sacc, facc, sr0, sr1, sr2, sr3, fr0, fr1, fr2, fr3, old_buf, spc, fpc,
                send_sem, recv_sem, loc_sem, old_sem, x_sem, h_sem, w_sem, sta_sem, stb_sem, z_sem, ainv_sem, sinv_sem, vt_sem, u_sem, u_send_sem, u_recv_sem):
    z_out = st_b
    me = lax.axis_index("data")
    core = lax.rem(me, 2)
    pos = [lax.rem(me // 2, 2), lax.rem(me // 4, 2), lax.rem(me // 8, 2)]
    core_peer = me + 1 - 2 * core
    peers = [me + (1 - 2 * pos[d]) * (2 << d) for d in range(3)]

    sym_recv = [sr0, sr1, sr2, sr3]
    full_recv = [fr0, fr1, fr2, fr3]

    def dims_of(g):
        return [g, (g + 1) % 3, (g + 2) % 3]

    def base_size(u, g):
        return (0, B) if u.kind == "sym" else u.groups[g]

    def offset(u, g, level):
        r0, n = base_size(u, g)
        bits = [core] + [pos[d] for d in dims_of(g)]
        off = r0
        for i in range(level):
            off = off + bits[i] * (n >> (i + 1))
        return pl.multiple_of(off, 8) if level else off

    def other(u, g, level):
        r0, n = base_size(u, g)
        bits = [core] + [pos[d] for d in dims_of(g)]
        return pl.multiple_of(offset(u, g, level) + (1 - bits[level]) * (n >> (level + 1)), 8)

    def peer(g, level):
        return core_peer if level == 0 else peers[dims_of(g)[level - 1]]

    def rows(u, g, level):
        return base_size(u, g)[1] >> level

    def acc_at(u, g, off, size):
        if u.kind == "sym":
            b0, nb = u.groups[g]
            return sacc.at[u.slot, pl.ds(b0, nb), pl.ds(off, size), :]
        return facc.at[u.slot, pl.ds(off, size), :]

    def recv_at(u, g, level, start=0, size=None):
        size = size or rows(u, g, level + 1)
        if u.kind == "sym":
            b0, nb = u.groups[g]
            return sym_recv[level].at[u.slot, pl.ds(b0, nb), pl.ds(start, size), :]
        return full_recv[level].at[u.slot, pl.ds((u.groups[g][0] >> (level + 1)) + start, size), :]

    def add_received(u, g, level):
        size = rows(u, g, level + 1)
        chunk = next(c for c in (32, 16, 8) if size % c == 0)
        mine = offset(u, g, level + 1)

        def body(i, carry):
            start = pl.multiple_of(i * chunk, 8)
            ref = acc_at(u, g, pl.multiple_of(mine + start, 8), chunk)
            ref[...] = ref[...] + recv_at(u, g, level, start, chunk)[...]
            return carry

        lax.fori_loop(0, size // chunk, body, 0)

    def piece_at(u, g):
        if u.kind == "sym":
            b0, nb = u.groups[g]
            return spc.at[u.slot, pl.ds(b0, nb)]
        r0, n = u.groups[g]
        return fpc.at[u.slot, pl.ds(r0 >> 4, n >> 4), :]

    def out_at(u, g, off, size):
        if u.kind == "sym":
            b0, nb = u.groups[g]
            return osym.at[u.out, pl.ds(b0, nb), pl.ds(off, size), :]
        return ovt.at[u.out, pl.ds(off, size), :]

    def sem_row(u):
        return u.slot if u.kind == "sym" else 3 + u.slot

    def rs_copy(u, g, level):
        return pltpu.make_async_remote_copy(
            src_ref=acc_at(u, g, other(u, g, level), rows(u, g, level + 1)), dst_ref=recv_at(u, g, level),
            send_sem=send_sem.at[sem_row(u), g], recv_sem=recv_sem.at[sem_row(u), level, g],
            device_id=(peer(g, level),), device_id_type=pl.DeviceIdType.MESH)

    def ag_copy(u, g, level):
        off, size = offset(u, g, level + 1), rows(u, g, level + 1)
        src = piece_at(u, g) if level == 3 else out_at(u, g, off, size)
        return pltpu.make_async_remote_copy(
            src_ref=src, dst_ref=out_at(u, g, off, size),
            send_sem=send_sem.at[sem_row(u), g], recv_sem=recv_sem.at[sem_row(u), 7 - level, g],
            device_id=(peer(g, level),), device_id_type=pl.DeviceIdType.MESH)

    def own_copy(u, g):
        return pltpu.make_async_copy(piece_at(u, g), out_at(u, g, offset(u, g, 4), rows(u, g, 4)), loc_sem.at[sem_row(u), g])

    def old_copies(u):
        src = aold_hbm if u.old == "a" else sold_hbm
        for g in range(3):
            b0, nb = u.groups[g]
            for b in range(b0, b0 + nb):
                bi, bj = SYM_BLOCKS[b]
                row = pl.multiple_of(bi * B + offset(u, g, 4), 8)
                for half in range(2):
                    from_row, from_col = row, bj * B + half * Q
                    if bi == bj and half == 0:
                        c_row, c_col = CARRIED[bi]
                        from_row = pl.multiple_of(row + core * ((3 - bi) * B - Q + c_row * Q), 8)
                        from_col = pl.multiple_of(from_col + core * ((3 - bi) * B + c_col * Q), Q)
                    pltpu.make_async_copy(src.at[u.layer, pl.ds(from_row, 16), pl.ds(from_col, Q)], old_buf.at[u.slot, b, :, pl.ds(half * Q, Q)], old_sem.at[u.slot]).start()

    def ainv_copy(layer):
        return pltpu.make_async_copy(ainv_hbm.at[layer], ainv_buf, ainv_sem)

    def event(u, e):
        if e == 0:
            if u.kind == "sym":
                for i, (c_row, c_col) in enumerate(CARRIED):
                    sacc[u.slot, DIAG[i], Q:, :Q] = sacc[u.slot, NB, c_row * Q:(c_row + 1) * Q, c_col * Q:(c_col + 1) * Q]
            for g in range(3):
                rs_copy(u, g, 0).start()
            if u.kind == "sym":
                old_copies(u)
            return
        if e <= 4:
            level = e - 1
            for g in range(3):
                rs_copy(u, g, level).wait_recv()
                rs_copy(u, g, level).wait_send()
                if e < 4:
                    add_received(u, g, level)
                    rs_copy(u, g, level + 1).start()
            if e == 4:
                if u.kind == "sym":
                    pltpu.make_async_copy(osym.at[u.out, :, pl.ds(0, 16), :], old_buf.at[u.slot], old_sem.at[u.slot]).wait()
                for g in range(3):
                    total = acc_at(u, g, offset(u, g, 4), rows(u, g, 4))[...] + recv_at(u, g, 3)[...]
                    if u.kind == "sym":
                        b0, nb = u.groups[g]
                        piece_at(u, g)[...] = RHO * old_buf[u.slot, pl.ds(b0, nb)] + (1.0 - RHO) * (total / tokens)
                    else:
                        piece_at(u, g)[...] = total / tokens
                if u.kind == "full":
                    ainv_copy(u.layer).wait()
                    fpc[u.slot] = dot_f32(fpc[u.slot], ainv_buf[...], precision=lax.Precision.HIGHEST)
                    if u.layer > 0:
                        ainv_copy(u.layer - 1).start()
                for g in range(3):
                    own_copy(u, g).start()
                    ag_copy(u, g, 3).start()
            return
        level = 8 - e
        for g in range(3):
            ag_copy(u, g, level).wait_recv()
            ag_copy(u, g, level).wait_send()
            if e == 5:
                own_copy(u, g).wait()
            if e < 8:
                ag_copy(u, g, level - 1).start()

    by_hook = {}
    for u in UNITS:
        for e, h in enumerate(u.hooks):
            by_hook.setdefault(h, []).append((u, e))

    def hook(index):
        for u, e in by_hook.get(index, []):
            event(u, e)

    def hooks_in_loop(phase, k):
        for i in range(NT):
            if by_hook.get(phase * NT + i):
                @pl.when(k == i)
                def _(i=i):
                    hook(phase * NT + i)

    def tile(k):
        return pl.ds(pl.multiple_of(k * tm, tm), tm)

    def x_copy(k):
        return pltpu.make_async_copy(x_hbm.at[tile(k), :], cur.at[tile(k), :], x_sem.at[k])

    def dy_copy(k, slot):
        return pltpu.make_async_copy(dy_hbm.at[tile(k), :], st_a.at[slot], sta_sem.at[slot])

    def hp_copy(layer, k, slot):
        src = x_hbm.at[tile(k), :] if layer == 0 else h_hbm.at[layer - 1, tile(k), :]
        return pltpu.make_async_copy(src, st_a.at[slot], sta_sem.at[slot])

    def zin_copy(layer, k, slot):
        return pltpu.make_async_copy(z_hbm.at[layer, tile(k), :], st_b.at[slot], stb_sem.at[slot])

    def zout_copy(layer, k, slot):
        return pltpu.make_async_copy(z_out.at[slot], z_hbm.at[layer, tile(k), :], z_sem.at[slot])

    def hout_copy(layer, k):
        return pltpu.make_async_copy(cur.at[tile(k), :], h_hbm.at[layer, tile(k), :], h_sem.at[k])

    def w_copy(layer, slot):
        return pltpu.make_async_copy(w_hbm.at[layer], w_buf.at[slot], w_sem.at[slot])

    def sym_add(slot, rows_t, rows_n):
        for j in range(4):
            part = dot_f32(rows_t[:B * (j + 1)], rows_n[:, B * j:B * (j + 1)]).reshape(j + 1, B, B)
            b0 = j * (j + 1) // 2
            sacc[slot, b0:b0 + j + 1] = sacc[slot, b0:b0 + j + 1] + part

    def full_add(slot, rows_t, read_cols):
        for j in range(4):
            cols = pl.ds(B * j, B)
            facc[slot, :, cols] = facc[slot, :, cols] + dot_f32(rows_t, read_cols(j))

    def loop(body):
        lax.fori_loop(0, NT, lambda k, c: (body(k), c)[1], 0)

    def clear_sym(slot):
        def body(i, carry):
            sacc[slot, i] = jnp.zeros((B, B), F32)
            return carry

        lax.fori_loop(0, NB + 1, body, 0)

    def clear_full(slot):
        def body(i, carry):
            facc[slot, pl.ds(pl.multiple_of(i * 64, 64), 64), :] = jnp.zeros((64, D), F32)
            return carry

        lax.fori_loop(0, D // 64, body, 0)

    for k in range(NT):
        x_copy(k).start()
    dy_copy(0, 0).start()
    w_copy(0, 0).start()
    w_copy(1, 1).start()

    barrier = pltpu.get_barrier_semaphore()
    for p in [core_peer] + peers:
        pl.semaphore_signal(barrier, inc=1, device_id=(p,), device_id_type=pl.DeviceIdType.MESH)
    pl.semaphore_wait(barrier, 4)

    clear_sym(0)
    clear_sym(1)

    def gram_dy(k):
        slot = lax.rem(k, 2)

        @pl.when(k + 1 < NT)
        def _():
            dy_copy(k + 1, 1 - slot).start()
        dy_copy(k, slot).wait()
        g = st_a[slot]
        sym_add(0, g.T, g)

    loop(gram_dy)

    def gram_x(k):
        hooks_in_loop(1, k)
        x_copy(k).wait()
        h = cur[tile(k), :]
        sym_add(1, h.T, h)

    loop(gram_x)

    for layer in range(3):
        phase = layer + 2
        wslot = layer % 2
        aslot = [2, 0, 1][layer]
        if layer > 0:
            w_copy(layer + 1, 1 - wslot).start()
        clear_sym(aslot)
        w_copy(layer, wslot).wait()

        def forward(k, layer=layer, phase=phase, wslot=wslot, aslot=aslot):
            hooks_in_loop(phase, k)
            slot = lax.rem(k, 2)

            @pl.when(k >= 2)
            def _():
                zout_copy(layer, k, slot).wait()
            h = cur[tile(k), :]
            for n in range(4):
                cols = pl.ds(B * n, B)
                z = dot_f32(h, w_buf[wslot, :, cols]).astype(BF16)
                z_out[slot, :, cols] = z
                zf = z.astype(F32)
                ht[:, cols] = (0.5 * zf * (1.0 + lax.erf(zf * ERF_SCALE))).astype(BF16)
            zout_copy(layer, k, slot).start()
            h2 = ht[...]
            sym_add(aslot, h2.T, h2)
            if layer > 0:
                hout_copy(layer - 1, k).wait()
            cur[tile(k), :] = ht[...]
            if layer < 2:
                hout_copy(layer, k).start()
            else:
                @pl.when(k == NT - 1)
                def _():
                    dy_copy(0, 0).start()

        loop(forward)
        zout_copy(layer, 0, 0).wait()
        zout_copy(layer, 1, 1).wait()

    clear_full(0)

    def top(k):
        hooks_in_loop(5, k)
        slot = lax.rem(k, 2)

        @pl.when(k + 1 < NT)
        def _():
            dy_copy(k + 1, 1 - slot).start()

        dy_copy(k, slot).wait()

        @pl.when(k == NT - 1)
        def _():
            hp_copy(2, 0, 0).start()
            zin_copy(2, 0, 0).start()

        g = st_a[slot]
        full_add(0, g.T, lambda j: cur[tile(k), pl.ds(B * j, B)])
        cur[tile(k), :] = st_a[slot]

    loop(top)

    for layer in (2, 1, 0):
        phase = 8 - layer
        wslot = [1, 0, 1][layer]
        sslot = [1, 0, 2][layer]
        fslot = [1, 0, 1][layer]
        if layer == 2:
            ainv_copy(3).start()
        if layer == 1:
            w_copy(1, 1).start()
        clear_sym(sslot)
        clear_full(fslot)
        if layer != 1:
            w_copy(layer + 1, wslot).wait()

        def backward(k, layer=layer, phase=phase, wslot=wslot, sslot=sslot, fslot=fslot):
            hooks_in_loop(phase, k)
            slot = lax.rem(k, 2)

            @pl.when(k + 1 < NT)
            def _():
                hp_copy(layer, k + 1, 1 - slot).start()
                zin_copy(layer, k + 1, 1 - slot).start()

            hp_copy(layer, k, slot).wait()
            zin_copy(layer, k, slot).wait()
            if layer > 0:
                @pl.when(k == NT - 1)
                def _():
                    hp_copy(layer - 1, 0, 0).start()
                    zin_copy(layer - 1, 0, 0).start()

            g_up = cur[tile(k), :]
            for n in range(4):
                cols = pl.ds(B * n, B)
                dh = dot_f32(g_up, w_buf[wslot, cols, :], ((1,), (1,))).astype(BF16)
                zf = st_b[slot, :, cols].astype(F32)
                slope = 0.5 * (1.0 + lax.erf(zf * ERF_SCALE)) + zf * jnp.exp(-0.5 * zf * zf) * PDF_SCALE
                ht[:, cols] = (dh.astype(F32) * slope).astype(BF16)
            g = ht[...]
            g_t = g.T
            sym_add(sslot, g_t, g)
            full_add(fslot, g_t, lambda j: st_a[slot, :, pl.ds(B * j, B)])
            cur[tile(k), :] = ht[...]

        loop(backward)

    first_last = 9 * NT
    n_last = max(max(max(u.hooks) for u in UNITS) + 1 - first_last, U_START + U_PIECES)

    def sinv_copy(layer):
        return pltpu.make_async_copy(sinv_hbm.at[layer], sinv_buf, sinv_sem)

    def vt_copy(layer, m, slot):
        return pltpu.make_async_copy(ovt.at[layer, :, pl.ds(pl.multiple_of(m * B, B), B)], vt_buf.at[slot], vt_sem.at[slot])

    def piece_of(p):
        return 3 - p // 2, 2 * lax.rem(p, 2) + core, lax.rem(p, 2)

    def u_at(layer, m):
        return u_hbm.at[layer, pl.ds(pl.multiple_of(m * B, B), B), :]

    def u_copy(layer, m):
        return pltpu.make_async_copy(u_buf, u_at(layer, m), u_sem)

    def u_send(layer, m, p):
        return pltpu.make_async_remote_copy(
            src_ref=u_buf, dst_ref=u_at(layer, m), send_sem=u_send_sem, recv_sem=u_recv_sem.at[p],
            device_id=(core_peer,), device_id_type=pl.DeviceIdType.MESH)

    sinv_copy(3).start()

    def final(s, carry):
        for i in range(n_last):
            if by_hook.get(first_last + i):
                @pl.when(s == i)
                def _(i=i):
                    hook(first_last + i)

        @pl.when((s + 1 >= U_START) & (s + 1 < U_START + U_PIECES))
        def _():
            vt_copy(*piece_of(s + 1 - U_START)).start()

        @pl.when((s >= U_START) & (s < U_START + U_PIECES))
        def _():
            p = s - U_START
            layer, m, slot = piece_of(p)

            @pl.when(slot == 0)
            def _():
                sinv_copy(layer).wait()

            vt_copy(layer, m, slot).wait()

            @pl.when(p > 0)
            def _():
                u_copy(layer, m).wait()
                u_send(layer, m, p).wait_send()
            for j in range(2):
                part = dot_f32(sinv_buf[512 * j:512 * (j + 1), :], vt_buf[slot], precision=lax.Precision.HIGHEST)
                u_buf[:, 512 * j:512 * (j + 1)] = part.T
            u_copy(layer, m).start()
            u_send(layer, m, p).start()

            @pl.when((slot == 1) & (layer > 0))
            def _():
                sinv_copy(layer - 1).start()
        return carry

    lax.fori_loop(0, n_last, final, 0)
    u_copy(0, core).wait()
    u_send(0, core, 0).wait_send()
    for p in range(U_PIECES):
        layer, m, _ = piece_of(p)
        u_send(layer, m, p).wait_recv()


def tail_kernel(sym_ref, u_ref, u_out, a_out, s_out):
    u_out[...] = u_ref[...]

    step = pl.program_id(0)

    def put(out_ref, half, row, col, blk):
        if row // (D // 2) == half:
            row = row - half * (D // 2)
            out_ref[0, row:row + blk.shape[0], col:col + blk.shape[1]] = blk

    def expand(out_ref, half):
        for b, (bi, bj) in enumerate(SYM_BLOCKS[:NB]):
            row, col = bi * B, bj * B
            if bi != bj:
                put(out_ref, half, row, col, sym_ref[0, b])
                put(out_ref, half, col, row, sym_ref[0, b].T)
            else:
                put(out_ref, half, row, col, sym_ref[0, b, :Q, :])
                put(out_ref, half, row + Q, col + Q, sym_ref[0, b, Q:, Q:])
                put(out_ref, half, row + Q, col, sym_ref[0, b, :Q, Q:].T)
                carried = sym_ref[0, b, Q:, :Q]
                c_row, c_col = CARRIED[bi]
                put(out_ref, half, 3 * B + c_row * Q, 3 * B + c_col * Q, carried)
                if c_row != c_col:
                    put(out_ref, half, 3 * B + c_col * Q, 3 * B + c_row * Q, carried.T)

    for half in range(2):
        @pl.when((step < 8) & (lax.rem(step, 2) == half))
        def _(half=half):
            expand(a_out, half)

        @pl.when((step >= 8) & (lax.rem(step, 2) == half))
        def _(half=half):
            expand(s_out, half)


def tail(osym, u_part):
    full = jax.ShapeDtypeStruct((4, D, D), F32)
    return pl.pallas_call(
        tail_kernel,
        grid=(16,),
        in_specs=[pl.BlockSpec((1, NB, B, B), lambda i: (i // 2, 0, 0, 0)), pl.BlockSpec((1, B, D), lambda i: (i // 4, i % 4, 0))],
        out_specs=(
            pl.BlockSpec((1, B, D), lambda i: (i // 4, i % 4, 0)),
            pl.BlockSpec((1, D // 2, D), lambda i: (jnp.minimum(i, 7) // 2, jnp.minimum(i, 7) % 2, 0)),
            pl.BlockSpec((1, D // 2, D), lambda i: (jnp.maximum(i - 8, 0) // 2, jnp.maximum(i - 8, 0) % 2, 0)),
        ),
        out_shape=(full, full, full),
        compiler_params=pltpu.CompilerParams(vmem_limit_bytes=48 * 1024 * 1024),
        name="tail_kernel",
    )(osym, u_part)


def solution(mesh):
    group_size = mesh.shape["data"]

    def local_step(x_loc, dy_loc, w_stack, a_old, s_old, a_inv, s_inv):
        n_rows = x_loc.shape[0]
        tm = n_rows // NT
        tokens = n_rows * group_size
        any_spec = pl.BlockSpec(memory_space=pl.ANY)
        vm = pltpu.VMEM
        osym, _, u_part, _, _ = pl.pallas_call(
            functools.partial(step_kernel, tm, float(tokens)),
            out_shape=(
                jax.ShapeDtypeStruct((8, NB, B, B), F32),
                jax.ShapeDtypeStruct((4, D, D), F32),
                jax.ShapeDtypeStruct((4, D, D), F32),
                jax.ShapeDtypeStruct((3, n_rows, D), BF16),
                jax.ShapeDtypeStruct((2, n_rows, D), BF16),
            ),
            in_specs=[any_spec] * 7,
            out_specs=(any_spec,) * 5,
            scratch_shapes=[
                vm((n_rows, D), BF16), vm((tm, D), BF16), vm((2, D, D), BF16), vm((2, tm, D), BF16), vm((2, tm, D), BF16),
                vm((D, D), F32), vm((D, D), F32), vm((2, D, B), F32), vm((B, D), F32),
                vm((3, NB + 1, B, B), F32), vm((2, D, D), F32),
                *[vm((3, NB, B >> i, B), F32) for i in range(1, 5)],
                *[vm((2, D >> i, D), F32) for i in range(1, 5)],
                vm((3, NB, 16, B), F32), vm((3, NB, 16, B), F32), vm((2, 64, D), F32),
                pltpu.SemaphoreType.DMA((5, 3)), pltpu.SemaphoreType.DMA((5, 8, 3)), pltpu.SemaphoreType.DMA((5, 3)),
                pltpu.SemaphoreType.DMA((3,)), pltpu.SemaphoreType.DMA((NT,)), pltpu.SemaphoreType.DMA((NT,)),
                pltpu.SemaphoreType.DMA((2,)), pltpu.SemaphoreType.DMA((2,)), pltpu.SemaphoreType.DMA((2,)),
                pltpu.SemaphoreType.DMA((2,)), pltpu.SemaphoreType.DMA, pltpu.SemaphoreType.DMA, pltpu.SemaphoreType.DMA((2,)), pltpu.SemaphoreType.DMA,
                pltpu.SemaphoreType.DMA, pltpu.SemaphoreType.DMA((U_PIECES,)),
            ],
            compiler_params=pltpu.CompilerParams(collective_id=0, has_side_effects=True, vmem_limit_bytes=67043328),
            name="step_kernel",
        )(x_loc, dy_loc, w_stack, a_old, s_old, a_inv, s_inv)
        return tail(osym, u_part)

    row_spec = P("data", None)
    full_spec = P()
    return jax.shard_map(local_step, mesh=mesh, in_specs=(row_spec, row_spec, full_spec, full_spec, full_spec, full_spec, full_spec), out_specs=(full_spec, full_spec, full_spec), check_vma=False)
```

```python
import functools

import jax
import jax.numpy as jnp
from jax import lax
from jax.experimental import pallas as pl
from jax.experimental.pallas import tpu as pltpu
from jax.sharding import PartitionSpec as P

RHO = 0.75
ERF_SCALE = 0.7071067811865476
PDF_SCALE = 0.3989422804014327
D = 1024
B = 256
NT = 8
F32 = jnp.float32
BF16 = jnp.bfloat16

SYM_BLOCKS = [(bi, bj) for bj in range(4) for bi in range(bj + 1)]
NB = len(SYM_BLOCKS) - 1
Q = B // 2
DIAG = [SYM_BLOCKS.index((i, i)) for i in range(4)]
CARRIED = [(0, 0), (0, 1), (1, 1)]


def dot_f32(lhs, rhs, dims=((1,), (0,)), precision=None):
    return lax.dot_general(lhs, rhs, (dims, ((), ())), precision=precision, preferred_element_type=F32)


class Unit:
    def __init__(self, kind, layer, slot, first, gaps, rot):
        self.kind, self.old, self.layer, self.slot = ("full" if kind == "w" else "sym"), kind, layer, slot
        self.out = layer + (4 if kind == "s" else 0)
        self.hooks = [first]
        for gap in gaps:
            self.hooks.append(self.hooks[-1] + int(gap))
        if self.kind == "sym":
            sizes = [3, 3, 3]
        else:
            sizes = [384, 384, 384]
            sizes[rot % 3] = 256
        starts = [0, sizes[0], sizes[0] + sizes[1]]
        self.groups = list(zip(starts, sizes))


U_PIECES = 8
U_START = 13

UNITS = [
    Unit("s", 0, 1, 77, "22214224", 0),
    Unit("w", 1, 0, 67, "28321131", 2),
    Unit("a", 3, 1, 42, "76223118", 0),
    Unit("w", 2, 1, 56, "23111246", 1),
    Unit("a", 1, 2, 28, "24522365", 0),
    Unit("w", 3, 0, 48, "23111244", 0),
    Unit("s", 1, 0, 65, "37713328", 0),
    Unit("a", 2, 0, 34, "27542130", 0),
    Unit("a", 0, 1, 17, "63223233", 0),
    Unit("w", 0, 1, 77, "31111321", 0),
    Unit("s", 2, 2, 61, "37734322", 0),
    Unit("s", 3, 0, 8, "83213233", 0),
]


def step_kernel(tm, tokens, x_hbm, dy_hbm, w_hbm, aold_hbm, sold_hbm, ainv_hbm, sinv_hbm,
                osym, ovt, u_hbm, z_hbm, h_hbm,
                cur, ht, w_buf, st_a, st_b, ainv_buf, sinv_buf, vt_buf, u_buf,
                sacc, facc, sr0, sr1, sr2, sr3, fr0, fr1, fr2, fr3, old_buf, spc, fpc,
                send_sem, recv_sem, loc_sem, old_sem, x_sem, h_sem, w_sem, sta_sem, stb_sem, z_sem, ainv_sem, sinv_sem, vt_sem, u_sem, u_send_sem, u_recv_sem):
    z_out = st_b
    me = lax.axis_index("data")
    core = lax.rem(me, 2)
    pos = [lax.rem(me // 2, 2), lax.rem(me // 4, 2), lax.rem(me // 8, 2)]
    core_peer = me + 1 - 2 * core
    peers = [me + (1 - 2 * pos[d]) * (2 << d) for d in range(3)]

    sym_recv = [sr0, sr1, sr2, sr3]
    full_recv = [fr0, fr1, fr2, fr3]

    def dims_of(g):
        return [g, (g + 1) % 3, (g + 2) % 3]

    def base_size(u, g):
        return (0, B) if u.kind == "sym" else u.groups[g]

    def offset(u, g, level):
        r0, n = base_size(u, g)
        bits = [core] + [pos[d] for d in dims_of(g)]
        off = r0
        for i in range(level):
            off = off + bits[i] * (n >> (i + 1))
        return pl.multiple_of(off, 8) if level else off

    def other(u, g, level):
        r0, n = base_size(u, g)
        bits = [core] + [pos[d] for d in dims_of(g)]
        return pl.multiple_of(offset(u, g, level) + (1 - bits[level]) * (n >> (level + 1)), 8)

    def peer(g, level):
        return core_peer if level == 0 else peers[dims_of(g)[level - 1]]

    def rows(u, g, level):
        return base_size(u, g)[1] >> level

    def acc_at(u, g, off, size):
        if u.kind == "sym":
            b0, nb = u.groups[g]
            return sacc.at[u.slot, pl.ds(b0, nb), pl.ds(off, size), :]
        return facc.at[u.slot, pl.ds(off, size), :]

    def recv_at(u, g, level, start=0, size=None):
        size = size or rows(u, g, level + 1)
        if u.kind == "sym":
            b0, nb = u.groups[g]
            return sym_recv[level].at[u.slot, pl.ds(b0, nb), pl.ds(start, size), :]
        return full_recv[level].at[u.slot, pl.ds((u.groups[g][0] >> (level + 1)) + start, size), :]

    def add_received(u, g, level):
        size = rows(u, g, level + 1)
        chunk = next(c for c in (32, 16, 8) if size % c == 0)
        mine = offset(u, g, level + 1)

        def body(i, carry):
            start = pl.multiple_of(i * chunk, 8)
            ref = acc_at(u, g, pl.multiple_of(mine + start, 8), chunk)
            ref[...] = ref[...] + recv_at(u, g, level, start, chunk)[...]
            return carry

        lax.fori_loop(0, size // chunk, body, 0)

    def piece_at(u, g):
        if u.kind == "sym":
            b0, nb = u.groups[g]
            return spc.at[u.slot, pl.ds(b0, nb)]
        r0, n = u.groups[g]
        return fpc.at[u.slot, pl.ds(r0 >> 4, n >> 4), :]

    def out_at(u, g, off, size):
        if u.kind == "sym":
            b0, nb = u.groups[g]
            return osym.at[u.out, pl.ds(b0, nb), pl.ds(off, size), :]
        return ovt.at[u.out, pl.ds(off, size), :]

    def sem_row(u):
        return u.slot if u.kind == "sym" else 3 + u.slot

    def rs_copy(u, g, level):
        return pltpu.make_async_remote_copy(
            src_ref=acc_at(u, g, other(u, g, level), rows(u, g, level + 1)), dst_ref=recv_at(u, g, level),
            send_sem=send_sem.at[sem_row(u), g], recv_sem=recv_sem.at[sem_row(u), level, g],
            device_id=(peer(g, level),), device_id_type=pl.DeviceIdType.MESH)

    def ag_copy(u, g, level):
        off, size = offset(u, g, level + 1), rows(u, g, level + 1)
        src = piece_at(u, g) if level == 3 else out_at(u, g, off, size)
        return pltpu.make_async_remote_copy(
            src_ref=src, dst_ref=out_at(u, g, off, size),
            send_sem=send_sem.at[sem_row(u), g], recv_sem=recv_sem.at[sem_row(u), 7 - level, g],
            device_id=(peer(g, level),), device_id_type=pl.DeviceIdType.MESH)

    def own_copy(u, g):
        return pltpu.make_async_copy(piece_at(u, g), out_at(u, g, offset(u, g, 4), rows(u, g, 4)), loc_sem.at[sem_row(u), g])

    def old_copies(u):
        src = aold_hbm if u.old == "a" else sold_hbm
        for g in range(3):
            b0, nb = u.groups[g]
            for b in range(b0, b0 + nb):
                bi, bj = SYM_BLOCKS[b]
                row = pl.multiple_of(bi * B + offset(u, g, 4), 8)
                for half in range(2):
                    from_row, from_col = row, bj * B + half * Q
                    if bi == bj and half == 0:
                        c_row, c_col = CARRIED[bi]
                        from_row = pl.multiple_of(row + core * ((3 - bi) * B - Q + c_row * Q), 8)
                        from_col = pl.multiple_of(from_col + core * ((3 - bi) * B + c_col * Q), Q)
                    pltpu.make_async_copy(src.at[u.layer, pl.ds(from_row, 16), pl.ds(from_col, Q)], old_buf.at[u.slot, b, :, pl.ds(half * Q, Q)], old_sem.at[u.slot]).start()

    def ainv_copy(layer):
        return pltpu.make_async_copy(ainv_hbm.at[layer], ainv_buf, ainv_sem)

    def event(u, e):
        if e == 0:
            if u.kind == "sym":
                for i, (c_row, c_col) in enumerate(CARRIED):
                    sacc[u.slot, DIAG[i], Q:, :Q] = sacc[u.slot, NB, c_row * Q:(c_row + 1) * Q, c_col * Q:(c_col + 1) * Q]
            for g in range(3):
                rs_copy(u, g, 0).start()
            if u.kind == "sym":
                old_copies(u)
            return
        if e <= 4:
            level = e - 1
            for g in range(3):
                rs_copy(u, g, level).wait_recv()
                rs_copy(u, g, level).wait_send()
                if e < 4:
                    add_received(u, g, level)
                    rs_copy(u, g, level + 1).start()
            if e == 4:
                if u.kind == "sym":
                    pltpu.make_async_copy(osym.at[u.out, :, pl.ds(0, 16), :], old_buf.at[u.slot], old_sem.at[u.slot]).wait()
                for g in range(3):
                    total = acc_at(u, g, offset(u, g, 4), rows(u, g, 4))[...] + recv_at(u, g, 3)[...]
                    if u.kind == "sym":
                        b0, nb = u.groups[g]
                        piece_at(u, g)[...] = RHO * old_buf[u.slot, pl.ds(b0, nb)] + (1.0 - RHO) * (total / tokens)
                    else:
                        piece_at(u, g)[...] = total / tokens
                if u.kind == "full":
                    ainv_copy(u.layer).wait()
                    fpc[u.slot] = dot_f32(fpc[u.slot], ainv_buf[...], precision=lax.Precision.HIGHEST)
                    if u.layer > 0:
                        ainv_copy(u.layer - 1).start()
                for g in range(3):
                    own_copy(u, g).start()
                    ag_copy(u, g, 3).start()
            return
        level = 8 - e
        for g in range(3):
            ag_copy(u, g, level).wait_recv()
            ag_copy(u, g, level).wait_send()
            if e == 5:
                own_copy(u, g).wait()
            if e < 8:
                ag_copy(u, g, level - 1).start()

    by_hook = {}
    for u in UNITS:
        for e, h in enumerate(u.hooks):
            by_hook.setdefault(h, []).append((u, e))

    def hook(index):
        for u, e in by_hook.get(index, []):
            event(u, e)

    def hooks_in_loop(phase, k):
        for i in range(NT):
            if by_hook.get(phase * NT + i):
                @pl.when(k == i)
                def _(i=i):
                    hook(phase * NT + i)

    def tile(k):
        return pl.ds(pl.multiple_of(k * tm, tm), tm)

    def x_copy(k):
        return pltpu.make_async_copy(x_hbm.at[tile(k), :], cur.at[tile(k), :], x_sem.at[k])

    def dy_copy(k, slot):
        return pltpu.make_async_copy(dy_hbm.at[tile(k), :], st_a.at[slot], sta_sem.at[slot])

    def hp_copy(layer, k, slot):
        src = x_hbm.at[tile(k), :] if layer == 0 else h_hbm.at[layer - 1, tile(k), :]
        return pltpu.make_async_copy(src, st_a.at[slot], sta_sem.at[slot])

    def zin_copy(layer, k, slot):
        return pltpu.make_async_copy(z_hbm.at[layer, tile(k), :], st_b.at[slot], stb_sem.at[slot])

    def zout_copy(layer, k, slot):
        return pltpu.make_async_copy(z_out.at[slot], z_hbm.at[layer, tile(k), :], z_sem.at[slot])

    def hout_copy(layer, k):
        return pltpu.make_async_copy(cur.at[tile(k), :], h_hbm.at[layer, tile(k), :], h_sem.at[k])

    def w_copy(layer, slot):
        return pltpu.make_async_copy(w_hbm.at[layer], w_buf.at[slot], w_sem.at[slot])

    def sym_add(slot, rows_t, rows_n):
        for j in range(4):
            part = dot_f32(rows_t[:B * (j + 1)], rows_n[:, B * j:B * (j + 1)]).reshape(j + 1, B, B)
            b0 = j * (j + 1) // 2
            sacc[slot, b0:b0 + j + 1] = sacc[slot, b0:b0 + j + 1] + part

    def full_add(slot, rows_t, read_cols):
        for j in range(4):
            cols = pl.ds(B * j, B)
            facc[slot, :, cols] = facc[slot, :, cols] + dot_f32(rows_t, read_cols(j))

    def loop(body):
        lax.fori_loop(0, NT, lambda k, c: (body(k), c)[1], 0)

    def clear_sym(slot):
        def body(i, carry):
            sacc[slot, i] = jnp.zeros((B, B), F32)
            return carry

        lax.fori_loop(0, NB + 1, body, 0)

    def clear_full(slot):
        def body(i, carry):
            facc[slot, pl.ds(pl.multiple_of(i * 64, 64), 64), :] = jnp.zeros((64, D), F32)
            return carry

        lax.fori_loop(0, D // 64, body, 0)

    for k in range(NT):
        x_copy(k).start()
    dy_copy(0, 0).start()
    w_copy(0, 0).start()
    w_copy(1, 1).start()

    barrier = pltpu.get_barrier_semaphore()
    for p in [core_peer] + peers:
        pl.semaphore_signal(barrier, inc=1, device_id=(p,), device_id_type=pl.DeviceIdType.MESH)
    pl.semaphore_wait(barrier, 4)

    clear_sym(0)
    clear_sym(1)

    def gram_dy(k):
        slot = lax.rem(k, 2)

        @pl.when(k + 1 < NT)
        def _():
            dy_copy(k + 1, 1 - slot).start()
        dy_copy(k, slot).wait()
        g = st_a[slot]
        sym_add(0, g.T, g)

    loop(gram_dy)

    def gram_x(k):
        hooks_in_loop(1, k)
        x_copy(k).wait()
        h = cur[tile(k), :]
        sym_add(1, h.T, h)

    loop(gram_x)

    for layer in range(3):
        phase = layer + 2
        wslot = layer % 2
        aslot = [2, 0, 1][layer]
        if layer > 0:
            w_copy(layer + 1, 1 - wslot).start()
        clear_sym(aslot)
        w_copy(layer, wslot).wait()

        def forward(k, layer=layer, phase=phase, wslot=wslot, aslot=aslot):
            hooks_in_loop(phase, k)
            slot = lax.rem(k, 2)

            @pl.when(k >= 2)
            def _():
                zout_copy(layer, k, slot).wait()
            h = cur[tile(k), :]
            for n in range(4):
                cols = pl.ds(B * n, B)
                z = dot_f32(h, w_buf[wslot, :, cols]).astype(BF16)
                z_out[slot, :, cols] = z
                zf = z.astype(F32)
                ht[:, cols] = (0.5 * zf * (1.0 + lax.erf(zf * ERF_SCALE))).astype(BF16)
            zout_copy(layer, k, slot).start()
            h2 = ht[...]
            sym_add(aslot, h2.T, h2)
            if layer > 0:
                hout_copy(layer - 1, k).wait()
            cur[tile(k), :] = ht[...]
            if layer < 2:
                hout_copy(layer, k).start()
            else:
                @pl.when(k == NT - 1)
                def _():
                    dy_copy(0, 0).start()

        loop(forward)
        zout_copy(layer, 0, 0).wait()
        zout_copy(layer, 1, 1).wait()

    clear_full(0)

    def top(k):
        hooks_in_loop(5, k)
        slot = lax.rem(k, 2)

        @pl.when(k + 1 < NT)
        def _():
            dy_copy(k + 1, 1 - slot).start()

        dy_copy(k, slot).wait()

        @pl.when(k == NT - 1)
        def _():
            hp_copy(2, 0, 0).start()
            zin_copy(2, 0, 0).start()

        g = st_a[slot]
        full_add(0, g.T, lambda j: cur[tile(k), pl.ds(B * j, B)])
        cur[tile(k), :] = st_a[slot]

    loop(top)

    for layer in (2, 1, 0):
        phase = 8 - layer
        wslot = [1, 0, 1][layer]
        sslot = [1, 0, 2][layer]
        fslot = [1, 0, 1][layer]
        if layer == 2:
            ainv_copy(3).start()
        if layer == 1:
            w_copy(1, 1).start()
        clear_sym(sslot)
        clear_full(fslot)
        if layer != 1:
            w_copy(layer + 1, wslot).wait()

        def backward(k, layer=layer, phase=phase, wslot=wslot, sslot=sslot, fslot=fslot):
            hooks_in_loop(phase, k)
            slot = lax.rem(k, 2)

            @pl.when(k + 1 < NT)
            def _():
                hp_copy(layer, k + 1, 1 - slot).start()
                zin_copy(layer, k + 1, 1 - slot).start()

            hp_copy(layer, k, slot).wait()
            zin_copy(layer, k, slot).wait()
            if layer > 0:
                @pl.when(k == NT - 1)
                def _():
                    hp_copy(layer - 1, 0, 0).start()
                    zin_copy(layer - 1, 0, 0).start()

            g_up = cur[tile(k), :]
            for n in range(4):
                cols = pl.ds(B * n, B)
                dh = dot_f32(g_up, w_buf[wslot, cols, :], ((1,), (1,))).astype(BF16)
                zf = st_b[slot, :, cols].astype(F32)
                slope = 0.5 * (1.0 + lax.erf(zf * ERF_SCALE)) + zf * jnp.exp(-0.5 * zf * zf) * PDF_SCALE
                ht[:, cols] = (dh.astype(F32) * slope).astype(BF16)
            g = ht[...]
            g_t = g.T
            sym_add(sslot, g_t, g)
            full_add(fslot, g_t, lambda j: st_a[slot, :, pl.ds(B * j, B)])
            cur[tile(k), :] = ht[...]

        loop(backward)

    first_last = 9 * NT
    n_last = max(max(max(u.hooks) for u in UNITS) + 1 - first_last, U_START + U_PIECES)

    def sinv_copy(layer):
        return pltpu.make_async_copy(sinv_hbm.at[layer], sinv_buf, sinv_sem)

    def vt_copy(layer, m, slot):
        return pltpu.make_async_copy(ovt.at[layer, :, pl.ds(pl.multiple_of(m * B, B), B)], vt_buf.at[slot], vt_sem.at[slot])

    def piece_of(p):
        return 3 - p // 2, 2 * lax.rem(p, 2) + core, lax.rem(p, 2)

    def u_at(layer, m):
        return u_hbm.at[layer, pl.ds(pl.multiple_of(m * B, B), B), :]

    def u_copy(layer, m):
        return pltpu.make_async_copy(u_buf, u_at(layer, m), u_sem)

    def u_send(layer, m, p):
        return pltpu.make_async_remote_copy(
            src_ref=u_buf, dst_ref=u_at(layer, m), send_sem=u_send_sem, recv_sem=u_recv_sem.at[p],
            device_id=(core_peer,), device_id_type=pl.DeviceIdType.MESH)

    sinv_copy(3).start()

    def final(s, carry):
        for i in range(n_last):
            if by_hook.get(first_last + i):
                @pl.when(s == i)
                def _(i=i):
                    hook(first_last + i)

        @pl.when((s + 1 >= U_START) & (s + 1 < U_START + U_PIECES))
        def _():
            vt_copy(*piece_of(s + 1 - U_START)).start()

        @pl.when((s >= U_START) & (s < U_START + U_PIECES))
        def _():
            p = s - U_START
            layer, m, slot = piece_of(p)

            @pl.when(slot == 0)
            def _():
                sinv_copy(layer).wait()

            vt_copy(layer, m, slot).wait()

            @pl.when(p > 0)
            def _():
                u_copy(layer, m).wait()
                u_send(layer, m, p).wait_send()
            for j in range(2):
                part = dot_f32(sinv_buf[512 * j:512 * (j + 1), :], vt_buf[slot], precision=lax.Precision.HIGHEST)
                u_buf[:, 512 * j:512 * (j + 1)] = part.T
            u_copy(layer, m).start()
            u_send(layer, m, p).start()

            @pl.when((slot == 1) & (layer > 0))
            def _():
                sinv_copy(layer - 1).start()
        return carry

    lax.fori_loop(0, n_last, final, 0)
    u_copy(0, core).wait()
    u_send(0, core, 0).wait_send()
    for p in range(U_PIECES):
        layer, m, _ = piece_of(p)
        u_send(layer, m, p).wait_recv()


def tail_kernel(sym_ref, u_ref, u_out, a_out, s_out):
    u_out[...] = u_ref[...]

    step = pl.program_id(0)

    def put(out_ref, half, row, col, blk):
        if row // (D // 2) == half:
            row = row - half * (D // 2)
            out_ref[0, row:row + blk.shape[0], col:col + blk.shape[1]] = blk

    def expand(out_ref, half):
        for b, (bi, bj) in enumerate(SYM_BLOCKS[:NB]):
            row, col = bi * B, bj * B
            if bi != bj:
                put(out_ref, half, row, col, sym_ref[0, b])
                put(out_ref, half, col, row, sym_ref[0, b].T)
            else:
                put(out_ref, half, row, col, sym_ref[0, b, :Q, :])
                put(out_ref, half, row + Q, col + Q, sym_ref[0, b, Q:, Q:])
                put(out_ref, half, row + Q, col, sym_ref[0, b, :Q, Q:].T)
                carried = sym_ref[0, b, Q:, :Q]
                c_row, c_col = CARRIED[bi]
                put(out_ref, half, 3 * B + c_row * Q, 3 * B + c_col * Q, carried)
                if c_row != c_col:
                    put(out_ref, half, 3 * B + c_col * Q, 3 * B + c_row * Q, carried.T)

    for half in range(2):
        @pl.when((step < 8) & (lax.rem(step, 2) == half))
        def _(half=half):
            expand(a_out, half)

        @pl.when((step >= 8) & (lax.rem(step, 2) == half))
        def _(half=half):
            expand(s_out, half)


def tail(osym, u_part):
    full = jax.ShapeDtypeStruct((4, D, D), F32)
    return pl.pallas_call(
        tail_kernel,
        grid=(16,),
        in_specs=[pl.BlockSpec((1, NB, B, B), lambda i: (i // 2, 0, 0, 0)), pl.BlockSpec((1, B, D), lambda i: (i // 4, i % 4, 0))],
        out_specs=(
            pl.BlockSpec((1, B, D), lambda i: (i // 4, i % 4, 0)),
            pl.BlockSpec((1, D // 2, D), lambda i: (jnp.minimum(i, 7) // 2, jnp.minimum(i, 7) % 2, 0)),
            pl.BlockSpec((1, D // 2, D), lambda i: (jnp.maximum(i - 8, 0) // 2, jnp.maximum(i - 8, 0) % 2, 0)),
        ),
        out_shape=(full, full, full),
        compiler_params=pltpu.CompilerParams(vmem_limit_bytes=48 * 1024 * 1024),
        name="tail_kernel",
    )(osym, u_part)


def solution(mesh):
    group_size = mesh.shape["data"]

    def local_step(x_loc, dy_loc, w_stack, a_old, s_old, a_inv, s_inv):
        n_rows = x_loc.shape[0]
        tm = n_rows // NT
        tokens = n_rows * group_size
        any_spec = pl.BlockSpec(memory_space=pl.ANY)
        vm = pltpu.VMEM
        osym, _, u_part, _, _ = pl.pallas_call(
            functools.partial(step_kernel, tm, float(tokens)),
            out_shape=(
                jax.ShapeDtypeStruct((8, NB, B, B), F32),
                jax.ShapeDtypeStruct((4, D, D), F32),
                jax.ShapeDtypeStruct((4, D, D), F32),
                jax.ShapeDtypeStruct((3, n_rows, D), BF16),
                jax.ShapeDtypeStruct((2, n_rows, D), BF16),
            ),
            in_specs=[any_spec] * 7,
            out_specs=(any_spec,) * 5,
            scratch_shapes=[
                vm((n_rows, D), BF16), vm((tm, D), BF16), vm((2, D, D), BF16), vm((2, tm, D), BF16), vm((2, tm, D), BF16),
                vm((D, D), F32), vm((D, D), F32), vm((2, D, B), F32), vm((B, D), F32),
                vm((3, NB + 1, B, B), F32), vm((2, D, D), F32),
                *[vm((3, NB, B >> i, B), F32) for i in range(1, 5)],
                *[vm((2, D >> i, D), F32) for i in range(1, 5)],
                vm((3, NB, 16, B), F32), vm((3, NB, 16, B), F32), vm((2, 64, D), F32),
                pltpu.SemaphoreType.DMA((5, 3)), pltpu.SemaphoreType.DMA((5, 8, 3)), pltpu.SemaphoreType.DMA((5, 3)),
                pltpu.SemaphoreType.DMA((3,)), pltpu.SemaphoreType.DMA((NT,)), pltpu.SemaphoreType.DMA((NT,)),
                pltpu.SemaphoreType.DMA((2,)), pltpu.SemaphoreType.DMA((2,)), pltpu.SemaphoreType.DMA((2,)),
                pltpu.SemaphoreType.DMA((2,)), pltpu.SemaphoreType.DMA, pltpu.SemaphoreType.DMA, pltpu.SemaphoreType.DMA((2,)), pltpu.SemaphoreType.DMA,
                pltpu.SemaphoreType.DMA, pltpu.SemaphoreType.DMA((U_PIECES,)),
            ],
            compiler_params=pltpu.CompilerParams(collective_id=0, has_side_effects=True, vmem_limit_bytes=67043328),
            name="step_kernel",
        )(x_loc, dy_loc, w_stack, a_old, s_old, a_inv, s_inv)
        return tail(osym, u_part)

    row_spec = P("data", None)
    full_spec = P()
    return jax.shard_map(local_step, mesh=mesh, in_specs=(row_spec, row_spec, full_spec, full_spec, full_spec, full_spec, full_spec), out_specs=(full_spec, full_spec, full_spec), check_vma=False)
```
